256 devices in a mesh: row: 32 (over z_hi, x, core), col: 8 (over y, z_lo).
Axes of the slice: x: 4, y: 4, z: 8 (z_hi: 4, z_lo: 2; z = z_hi * 2 + z_lo), core: 2. Of those that a mesh axis runs over, the one named last changes fastest.
Arguments:
- pivots: int32 [256], replicated, may hold values from 0 to 32767, as said below
- panel: float32 [32768, 256], P(('row', 'col')), may hold values from -6 to 6
- prior: bfloat16 [32768, 3072], P(('row', 'col')), may hold values from -0.796875 to 0.796875
- finished: bfloat16 [32768, 256], P(('row', 'col')), may hold values from -6 to 6
- pairs: int32 [32768], replicated, may hold values from 0 to 639999, as said below
- occupied: bfloat16 [800, 120], replicated, may hold values from -0.21875 to 0.21875
Outputs:
- updated: float32 [32768, 256], P(('row', 'col'))
- halves: float32 [256, 120, 800], P(('row', 'col'))
The draws below stay inside these ranges and needn't reach their ends.
Inputs may be any that keep to these rules, and one draw needn't show every extreme that they name: `pivots`: distinct rows; at most 2 of them lie among the rows of one device (aligned blocks of 128 rows), and one device holds exactly 2. `pairs`: each value a * 800 + b with 0 <= b <= a < 800; all distinct and increasing.
All inputs are finite; a program needn't handle non-finite values.
Results may differ from the reference program's by a relative error of at most 0.0003.
Values may be sent and summed in bfloat16 or wider, within the bound.
A program may use at most 64 MiB of HBM per device.

```python
import jax
import jax.numpy as jnp
from jax import lax

K = 3072
PIVOTS = 256
NAO = 800
NOCC = 120
ROWS_DEV = 128
PAIRS = 32768
PIV_MOST = 2
DEVICES = 256


def draw_pivots(key, part):
    key_full, key_score, key_offset, key_shuffle = jax.random.split(jax.random.fold_in(key, 11), 4)
    total_slots = DEVICES * PIV_MOST
    full_block = jax.random.randint(key_full, (), 0, DEVICES)
    slot_ids = jnp.arange(total_slots, dtype=jnp.int32)
    scores = jax.random.permutation(key_score, total_slots).astype(jnp.int32)
    scores = jnp.where(slot_ids // PIV_MOST == full_block, -1 - slot_ids % PIV_MOST, scores)
    ordering = jnp.argsort(scores, stable=True)
    chosen = ordering[:PIVOTS].astype(jnp.int32)
    spacing = ROWS_DEV // PIV_MOST
    offsets = chosen % PIV_MOST * spacing + jax.random.randint(key_offset, (PIVOTS,), 0, spacing)
    result = chosen // PIV_MOST * ROWS_DEV + offsets
    return jax.random.permutation(key_shuffle, result).astype(jnp.int32)


def draw_pairs(key, part):
    total = NAO * (NAO + 1) // 2
    picked = jax.random.permutation(jax.random.fold_in(key, 23), total)[:PAIRS].astype(jnp.int32)
    picked = jnp.sort(picked)
    counter = jnp.arange(NAO, dtype=jnp.int32)
    starts = counter * (counter + 1) // 2
    first_ao = jnp.searchsorted(starts[1:], picked, side='right').astype(jnp.int32)
    second_ao = picked - jnp.take(starts, first_ao)
    return (first_ao * NAO + second_ao).astype(jnp.int32)


def block_scale(stream_key, dims, pieces, low, largest):
    def one(dim, blocks):
        steps = jax.random.uniform(jax.random.fold_in(jax.random.fold_in(stream_key, 6), dim), (blocks,), jnp.float32, low / len(pieces), largest / len(pieces))
        return jnp.repeat(jnp.exp(steps), dims[dim] // blocks).reshape((-1,) + (1,) * (len(dims) - dim - 1))

    factor_of = one(*pieces[0])
    for cut in pieces[1:]:
        factor_of = factor_of * one(*cut)
    return factor_of


def normal_values(own_key, extent, deviation, most, cuts=(), kind=jnp.bfloat16):
    values = jax.random.normal(own_key, extent, jnp.float32) * deviation
    if len(cuts) > 0:
        values = block_scale(own_key, extent, cuts, -0.22, 0.18) * values
    return jnp.clip(values, min=-most, max=most).astype(kind)


def setup_inputs(seed: int = 0) -> dict:
    seeds = jax.random.split(jax.random.key(seed), 7)
    pivots = draw_pivots(jax.random.fold_in(seeds[6], 71), 0)
    panel = normal_values(seeds[1], (PAIRS, PIVOTS), 1.0, 6.0, ((0, 256),), jnp.float32)
    prior = normal_values(seeds[2], (PAIRS, K), 0.134, 0.796875, ((0, 256),))
    finished = normal_values(seeds[3], (PAIRS, PIVOTS), 1.0, 6.0, ((0, 256),))
    pairs = draw_pairs(jax.random.fold_in(seeds[6], 71), 0)
    occupied = normal_values(seeds[5], (NAO, NOCC), NAO ** -0.5, 0.21875)
    return dict(pivots=pivots, panel=panel, prior=prior, finished=finished, pairs=pairs, occupied=occupied)


def build_matrix(column, pair_ids, mirrored, off_diag):
    matrix = jnp.zeros((NAO * NAO,), jnp.bfloat16)
    matrix = matrix.at[pair_ids].add(column)
    matrix = matrix.at[mirrored].add(jnp.where(off_diag, column, jnp.zeros_like(column)))
    return matrix.reshape(NAO, NAO)


def reference(pivots, panel, prior, finished, pairs, occupied):
    pivot_rows = jnp.take(prior, pivots, axis=0)
    updated = panel - jnp.dot(prior, pivot_rows.T, preferred_element_type=jnp.float32)
    first_ao = pairs // NAO
    second_ao = pairs % NAO
    mirrored = (second_ao * NAO + first_ao).astype(jnp.int32)
    off_diag = first_ao != second_ao

    def one_vector(column):
        matrix = build_matrix(column, pairs, mirrored, off_diag)
        return jnp.dot(occupied.T, matrix, preferred_element_type=jnp.float32)

    halves = lax.map(one_vector, finished.T)
    return updated, halves
```

```python
import functools
from collections import namedtuple

import jax
import jax.numpy as jnp
from jax import lax
from jax.experimental import pallas as pl
from jax.experimental.pallas import tpu as pltpu
from jax.sharding import PartitionSpec as P

MESH = pl.DeviceIdType.MESH
BF, F32, I32 = jnp.bfloat16, jnp.float32, jnp.int32
Dims = namedtuple("Dims", ("x", "y", "zh", "zl", "c"))
FULL = Dims(4, 4, 4, 2, 2)

NAO = 800
GROUP = 64
BLOCK = 256
TILE_ROWS = 2912
GROUPS = 46
UNROLL = 8

UNIT_TILES = (4, 4, 4)
UNIT_ORDERS = (("x", "y", "z"), ("y", "z", "x"), ("z", "x", "y"))


def nt(a, b):
    return lax.dot_general(a, b, (((1,), (1,)), ((), ())), preferred_element_type=F32)


def nn(a, b):
    return lax.dot_general(a, b, (((1,), (0,)), ((), ())), preferred_element_type=F32)


def iota(shape, dim):
    return lax.broadcasted_iota(I32, shape, dim)


def log2(n):
    assert n & (n - 1) == 0
    return n.bit_length() - 1


def mod(v, n):
    return v & (n - 1)


def div(v, n):
    return v >> log2(n)


def onehot(cond):
    return jnp.where(cond, 1.0, 0.0).astype(BF)


def coordinates(dims, device):
    col = mod(device, dims.y * dims.zl)
    row = div(device, dims.y * dims.zl)
    core = mod(row, dims.c)
    x = mod(div(row, dims.c), dims.x)
    zh = div(row, dims.c * dims.x)
    return dict(x=x, y=div(col, dims.zl), z=zh * dims.zl + mod(col, dims.zl), c=core)


def mesh_id(dims, p):
    row = (div(p["z"], dims.zl) * dims.x + p["x"]) * dims.c + p["c"]
    col = p["y"] * dims.zl + mod(p["z"], dims.zl)
    return (row, col)


class Plan:
    def __init__(self, dims, k, rows):
        self.dims = dims
        self.size = dict(x=dims.x, y=dims.y, z=dims.zh * dims.zl, c=dims.c)
        self.n = dims.x * dims.y * dims.zh * dims.zl * dims.c
        self.slots = 2 * self.n
        self.kt_half = k // 128 // 2
        self.rows = rows
        self.units = []
        first = 0
        for tiles, order in zip(UNIT_TILES, UNIT_ORDERS):
            self.units.append(
                dict(
                    tiles=tiles,
                    first=first,
                    order=order,
                    r1=-(-4 * tiles // 8) * 8,
                    n=[self.size[a] for a in order],
                )
            )
            first += tiles
        assert first == self.kt_half
        self.plane = dims.x * dims.y
        self.pole = self.size["z"] * dims.c


def move(me, **changes):
    return {**me, **changes}


def comm_kernel(plan, *refs):
    dims, size, n = plan.dims, plan.size, plan.n
    nu = len(plan.units)
    (piv_col, piv_row, prior, finished, out, vectors) = refs[:6]
    scratch = list(refs[6:])
    take = lambda count: [scratch.pop(0) for _ in range(count)]
    first_out = take(nu)
    first_in = take(nu)
    gathered = take(nu)
    (partner_prior, part_out, part_in, a_out, a_in, b_out, b_in) = take(7)
    (send1, recv1, send2, recv2, send3, recv3, send_a, recv_a, send_b, recv_b,
     send_p, recv_p, send_q, recv_q) = take(14)

    own = lax.axis_index("row") * (dims.y * dims.zl) + lax.axis_index("col")
    me = coordinates(dims, own)
    core = me["c"]
    other = move(me, c=1 - core)

    def step(axis, by):
        return mod(me[axis] + by, size[axis])

    lines = []
    for axis in ("x", "y", "z"):
        for by in range(1, size[axis]):
            for c in (core, 1 - core):
                lines.append(move(me, **{axis: step(axis, by), "c": c}))
    plane_peers = []
    for bx in range(dims.x):
        for by in range(dims.y):
            if bx or by:
                plane_peers.append(move(me, x=step("x", bx), y=step("y", by)))
    corners = []
    for bx in range(1, dims.x):
        for by in range(1, dims.y):
            corners.append(move(me, x=step("x", bx), y=step("y", by)))
    pole_peers = []
    for bz in range(size["z"]):
        for c in (core, 1 - core):
            if bz or c is not core:
                pole_peers.append(move(me, z=step("z", bz), c=c))
    peers = lines + corners + [other]

    barrier = pltpu.get_barrier_semaphore()
    for p in peers:
        pl.semaphore_signal(barrier, inc=1, device_id=mesh_id(dims, p), device_id_type=MESH)

    def remote(src, dst, send, recv, p):
        copy = pltpu.make_async_remote_copy(
            src_ref=src, dst_ref=dst, send_sem=send, recv_sem=recv,
            device_id=mesh_id(dims, p), device_id_type=MESH,
        )
        copy.start()

    def wait_bytes(ref, sem):
        pltpu.make_async_copy(ref, ref, sem).wait()

    npiv = piv_col.shape[0]
    here = onehot(piv_col[...] == own * plan.rows + iota((npiv, plan.rows), 1))
    has = nn(jnp.ones((32, npiv), BF), here)
    before = onehot(iota((plan.rows, plan.rows), 0) < iota((plan.rows, plan.rows), 1))
    rank = nn(has.astype(BF), before)
    q = iota((32, plan.rows), 0)
    wanted = (mod(q, 4) - core * 2).astype(F32)
    select = jnp.where((has > 0.5) & (rank == wanted), 1.0, 0.0).astype(BF)
    for h in range(2):
        for u, unit in enumerate(plan.units):
            k0 = (h * plan.kt_half + unit["first"]) * 128
            rows = nn(select, prior[:, k0 : k0 + unit["tiles"] * 128])
            r1 = unit["r1"]
            part = jnp.zeros((r1, 128), F32)
            which = div(iota((r1, 128), 0), 4)
            for kt in range(unit["tiles"]):
                part = jnp.where(which == kt, rows[:r1, kt * 128 : (kt + 1) * 128], part)
            first_out[u][h] = part.astype(BF)
    for u, unit in enumerate(plan.units):
        first_in[u][me[unit["order"][0]] * dims.c + core] = first_out[u][core]

    r = iota((n, n), 0)
    v = coordinates(dims, iota((n, n), 1))
    spot = ((v["x"] * dims.y + v["y"]) * size["z"] + v["z"]) * dims.c + v["c"]
    a_rows = nt(onehot(r == spot), finished[...]).astype(BF)
    for i in range(plan.plane):
        a_out[i] = a_rows[i * plan.pole : (i + 1) * plan.pole]
    my_plane = me["x"] * dims.y + me["y"]
    my_pole = me["z"] * dims.c + core
    a_in[my_plane] = a_out[my_plane]

    pl.semaphore_wait(barrier, len(peers))

    for p in plane_peers:
        remote(a_out.at[p["x"] * dims.y + p["y"]], a_in.at[my_plane], send_a, recv_a, p)
    for u, unit in enumerate(plan.units):
        axis = unit["order"][0]
        for by in range(size[axis]):
            for c in (core, 1 - core):
                if by or c is not core:
                    remote(
                        first_out[u].at[c], first_in[u].at[me[axis] * dims.c + core],
                        send1.at[u], recv1.at[u], move(me, **{axis: step(axis, by), "c": c}),
                    )
    half = plan.kt_half * 128
    remote(
        prior.at[:, pl.ds(pl.multiple_of((1 - core) * half, half), half)],
        partner_prior, send_p, recv_p, other,
    )

    wait_bytes(a_in.at[pl.ds(0, plan.plane - 1)], recv_a)
    mixed = a_in[...].reshape(n, plan.rows)
    source = mod(r, plan.plane) * plan.pole + div(r, plan.plane)
    b_rows = nn(onehot(iota((n, n), 1) == source), mixed).astype(BF)
    for i in range(plan.pole):
        b_out[i] = b_rows[i * plan.plane : (i + 1) * plan.plane]
    b_in[my_pole] = b_out[my_pole]
    for p in pole_peers:
        remote(b_out.at[p["z"] * dims.c + p["c"]], b_in.at[my_pole], send_b, recv_b, p)

    sends2 = []
    for u, unit in enumerate(plan.units):
        n1, n2, n3 = unit["n"]
        a1, a2, a3 = unit["order"]
        r1, tiles = unit["r1"], unit["tiles"]
        wait_bytes(first_in[u].at[pl.ds(0, n1 * dims.c - 1)], recv1.at[u])
        got = first_in[u][...].reshape(n1 * dims.c * r1, 128)
        shape = (tiles * n1 * 4, n1 * dims.c * r1)
        ro, ci = iota(shape, 0), iota(shape, 1)
        kt, slot = div(ro, n1 * 4), mod(ro, 4)
        target = (mod(div(ro, 4), n1) * dims.c + div(slot, 2)) * r1 + kt * 4 + slot
        rows = nn(onehot(ci == target), got).astype(BF)
        base = pl.multiple_of((me[a3] * n2 + me[a2]) * (n1 * 4), n1 * 4)
        for t in range(tiles):
            gathered[u][t, pl.ds(base, n1 * 4)] = rows[t * n1 * 4 : (t + 1) * n1 * 4]
        block = gathered[u].at[:, pl.ds(base, n1 * 4)]
        for by in range(1, n2):
            remote(block, block, send2.at[u], recv2.at[u], move(me, **{a2: step(a2, by)}))
        sends2.append((n1 * 4) * (n2 - 1))

    for u, unit in enumerate(plan.units):
        n1, n2, n3 = unit["n"]
        a3 = unit["order"][2]
        wait_bytes(gathered[u].at[:, pl.ds(0, sends2[u])], recv2.at[u])
        base = pl.multiple_of(me[a3] * (n2 * n1 * 4), n2 * n1 * 4)
        block = gathered[u].at[:, pl.ds(base, n2 * n1 * 4)]
        for by in range(1, n3):
            remote(block, block, send3.at[u], recv3.at[u], move(me, **{a3: step(a3, by)}))

    wait_bytes(b_in.at[pl.ds(0, plan.pole - 1)], recv_b)
    mixed = b_in[...].reshape(n, plan.rows)
    w = coordinates(dims, r)
    source = (w["z"] * dims.c + w["c"]) * plan.plane + w["x"] * dims.y + w["y"]
    vectors[...] = nn(onehot(iota((n, n), 1) == source), mixed)

    owner_c = div(piv_col[...], plan.rows)
    owner_r = div(piv_row[...], plan.rows)
    lower = onehot((owner_c == owner_r) & (piv_row[...] < piv_col[...]))
    place = nn(lower, jnp.ones((npiv, 128), BF)).astype(I32)
    o = coordinates(dims, jnp.broadcast_to(owner_c, (npiv, 128)))

    wait_bytes(partner_prior, recv_p)
    mine = jnp.zeros((plan.rows, npiv), F32)
    theirs = jnp.zeros((plan.rows, npiv), F32)
    for u, unit in enumerate(plan.units):
        n1, n2, n3 = unit["n"]
        a1, a2, a3 = unit["order"]
        wait_bytes(gathered[u].at[:, pl.ds(0, n2 * n1 * 4 * (n3 - 1))], recv3.at[u])
        line = ((o[a3] * n2 + o[a2]) * n1 + o[a1]) * 4 + o["c"] * 2 + place
        pick = jnp.concatenate(
            [onehot(iota((npiv, 128), 1) + s == line) for s in range(0, plan.slots, 128)], axis=1
        )
        if plan.slots < 128:
            pick = pick[:, : plan.slots]
        for t in range(unit["tiles"]):
            rows = nn(pick, gathered[u][t]).astype(BF)
            k0 = (unit["first"] + t) * 128
            mine += nt(prior[:, pl.ds(pl.multiple_of(core * half + k0, 128), 128)], rows)
            theirs += nt(partner_prior[:, k0 : k0 + 128], rows)
    part_out[...] = theirs
    remote(part_out, part_in, send_q, recv_q, other)

    for u, unit in enumerate(plan.units):
        n1, n2, n3 = unit["n"]
        wait_bytes(first_in[u].at[pl.ds(0, n1 * dims.c - 1)], send1.at[u])
        wait_bytes(gathered[u].at[:, pl.ds(0, sends2[u])], send2.at[u])
        wait_bytes(gathered[u].at[:, pl.ds(0, n2 * n1 * 4 * (n3 - 1))], send3.at[u])
    wait_bytes(a_in.at[pl.ds(0, plan.plane - 1)], send_a)
    wait_bytes(b_in.at[pl.ds(0, plan.pole - 1)], send_b)
    wait_bytes(partner_prior, send_p)
    wait_bytes(part_in, recv_q)
    wait_bytes(part_out, send_q)
    out[...] = mine + part_in[...]


def communicate(plan, pivots, prior, finished):
    npiv = pivots.shape[0]
    vmem = pl.BlockSpec(memory_space=pltpu.VMEM)
    dma = pltpu.SemaphoreType.DMA
    nu = len(plan.units)
    n, rows = plan.n, plan.rows
    scratch = [pltpu.VMEM((2, u["r1"], 128), BF) for u in plan.units]
    scratch += [pltpu.VMEM((u["n"][0] * plan.dims.c, u["r1"], 128), BF) for u in plan.units]
    scratch += [pltpu.VMEM((u["tiles"], plan.slots, 128), BF) for u in plan.units]
    scratch += [
        pltpu.VMEM((rows, plan.kt_half * 128), BF),
        pltpu.VMEM((rows, npiv), F32),
        pltpu.VMEM((rows, npiv), F32),
        pltpu.VMEM((plan.plane, plan.pole, rows), BF),
        pltpu.VMEM((plan.plane, plan.pole, rows), BF),
        pltpu.VMEM((plan.pole, plan.plane, rows), BF),
        pltpu.VMEM((plan.pole, plan.plane, rows), BF),
    ]
    scratch += [dma((nu,))] * 6 + [dma] * 8
    return pl.pallas_call(
        functools.partial(comm_kernel, plan),
        out_shape=(
            jax.ShapeDtypeStruct((rows, npiv), F32),
            jax.ShapeDtypeStruct((n, rows), F32),
        ),
        in_specs=[vmem] * 4,
        out_specs=(vmem, vmem),
        scratch_shapes=scratch,
        compiler_params=pltpu.CompilerParams(
            collective_id=0, has_side_effects=True, vmem_limit_bytes=40 * 1024 * 1024
        ),
        name="exchange",
    )(pivots.reshape(npiv, 1), pivots.reshape(1, npiv), prior, finished)


def group_of(pair):
    first = pair // NAO
    second = pair % NAO
    block = first >> 7
    return (block * (block + 1) * 64 + (first & 127) * (block + 1) + (second >> 7)) >> log2(GROUP)


def half_kernel(last, pairs, vector, occ_t, out, lane, line, tiles, dense, seq_g, seq_b):
    blocks = last.shape[0]
    steps = GROUPS + blocks - 1
    total = -(-steps // UNROLL) * UNROLL

    def schedule(t, state):
        g, b = state
        seq_g[t] = g
        seq_b[t] = b
        leave = (group_of(last[b]) > g) | (b == blocks - 1)
        return jnp.where(leave, g + 1, g), jnp.where(leave, b, b + 1)

    lax.fori_loop(0, total, schedule, (jnp.int32(0), jnp.int32(0)))

    flat = pairs[...].astype(F32)
    first = jnp.floor((flat + 0.5) * (1.0 / NAO)).astype(I32)
    second = pairs[...] - first * NAO
    row_block = first >> 7
    lane[...] = second & 127
    line[...] = (
        row_block * (row_block + 1) * 64 + (first & 127) * (row_block + 1) + (second >> 7)
    )

    lanes = iota((128, 128), 0)
    places = iota((GROUP, 128), 0)

    def some_steps(it, carry):
        acc, before = carry
        for k in range(UNROLL):
            t = it * UNROLL + k
            g, b = seq_g[t], seq_b[t]
            spread, where = [], []
            for j in range(2):
                at = pl.ds(2 * b + j, 1)
                spread.append(
                    jnp.where(lanes == lane[at, :], vector[at, :], 0.0).astype(BF)
                )
                where.append(onehot(places == line[at, :] - g * GROUP))
            new = nt(jnp.concatenate(spread, 1), jnp.concatenate(where, 1))
            acc = jnp.where(g == before, acc, 0.0) + new
            tiles[g] = acc
            before = g
        return acc, before

    lax.fori_loop(
        0, total // UNROLL, some_steps, (jnp.zeros((128, GROUP), F32), jnp.int32(-1))
    )

    for g in range(0, GROUPS, 2):
        pair = jnp.concatenate([tiles[g], tiles[g + 1]], axis=1)
        dense[g * GROUP : (g + 2) * GROUP, :] = pair.T

    wide = []
    for big in range(7):
        count = min(128, NAO - big * 128)
        base = 64 * big * (big + 1)
        row = []
        for c in range(big + 1):
            row.append(dense[pl.ds(base + c, count, stride=big + 1), :].astype(BF))
        wide.append(row)
    acc = [None] * 7
    for big in range(7):
        row = wide[big]
        count = row[0].shape[0]
        occ_rows = occ_t[:, big * 128 : big * 128 + count]
        for c in range(big + 1):
            term = nn(occ_rows, row[c])
            acc[c] = term if acc[c] is None else acc[c] + term
    for big in range(7):
        row = wide[big]
        count = row[0].shape[0]
        same = iota((count, 128), 0) == iota((count, 128), 1)
        row = row[:-1] + [jnp.where(same, jnp.zeros((), BF), row[-1])]
        full = row[0] if big == 0 else jnp.concatenate(row, axis=1)
        term = nt(occ_t[:, : (big + 1) * 128], full)
        total_block = acc[big][:, :count] + term
        out[:, big * 128 : big * 128 + count] = total_block[: out.shape[0]]


def half_transform(vector, pairs, occupied):
    vmem = pl.BlockSpec(memory_space=pltpu.VMEM)
    count, nocc = pairs.shape[0], occupied.shape[1]
    blocks = count // BLOCK
    last = pairs.reshape(blocks, BLOCK)[:, -1]
    occ_t = jnp.pad(occupied.T, ((0, 128 - nocc), (0, 896 - NAO)))
    total = -(-(GROUPS + blocks - 1) // UNROLL) * UNROLL
    return pl.pallas_call(
        half_kernel,
        out_shape=jax.ShapeDtypeStruct((nocc, NAO), F32),
        in_specs=[pl.BlockSpec(memory_space=pltpu.SMEM), vmem, vmem, vmem],
        out_specs=vmem,
        scratch_shapes=[
            pltpu.VMEM((count // 128, 128), I32),
            pltpu.VMEM((count // 128, 128), I32),
            pltpu.VMEM((GROUPS + UNROLL, 128, GROUP), F32),
            pltpu.VMEM((GROUPS * GROUP, 128), F32),
            pltpu.SMEM((total,), I32),
            pltpu.SMEM((total,), I32),
        ],
        compiler_params=pltpu.CompilerParams(vmem_limit_bytes=40 * 1024 * 1024),
        name="half",
    )(last, pairs.reshape(count // 128, 128), vector, occ_t)


def per_device(dims, pivots, panel, prior, finished, pairs, occupied):
    plan = Plan(dims, prior.shape[1], prior.shape[0])
    product, vector = communicate(plan, pivots, prior, finished)
    halves = half_transform(vector, pairs, occupied)
    return panel - product, halves[None]


def build(mesh, dims):
    return jax.shard_map(
        functools.partial(per_device, dims),
        mesh=mesh,
        in_specs=(
            P(),
            P(("row", "col"), None),
            P(("row", "col"), None),
            P(("row", "col"), None),
            P(),
            P(),
        ),
        out_specs=(P(("row", "col"), None), P(("row", "col"), None, None)),
        check_vma=False,
    )


def solution(mesh):
    return build(mesh, FULL)
```

```python
import functools
from collections import namedtuple

import jax
import jax.numpy as jnp
from jax import lax
from jax.experimental import pallas as pl
from jax.experimental.pallas import tpu as pltpu
from jax.sharding import PartitionSpec as P

MESH = pl.DeviceIdType.MESH
BF, F32, I32 = jnp.bfloat16, jnp.float32, jnp.int32
Dims = namedtuple("Dims", ("x", "y", "zh", "zl", "c"))
FULL = Dims(4, 4, 4, 2, 2)

NAO = 800
GROUP = 64
BLOCK = 256
GROUPS = 46
UNROLL = 8
MASK_UNROLL = 4

UNIT_TILES = (2, 5, 5)
UNIT_ORDERS = (("x", "y", "z"), ("y", "z", "x"), ("z", "x", "y"))


def nt(a, b):
    return lax.dot_general(a, b, (((1,), (1,)), ((), ())), preferred_element_type=F32)


def nn(a, b):
    return lax.dot_general(a, b, (((1,), (0,)), ((), ())), preferred_element_type=F32)


def iota(shape, dim):
    return lax.broadcasted_iota(I32, shape, dim)


def log2(n):
    assert n & (n - 1) == 0
    return n.bit_length() - 1


def mod(v, n):
    return v & (n - 1)


def div(v, n):
    return v >> log2(n)


def onehot(cond):
    return jnp.where(cond, 1.0, 0.0).astype(BF)


def coordinates(dims, device):
    col = mod(device, dims.y * dims.zl)
    row = div(device, dims.y * dims.zl)
    core = mod(row, dims.c)
    x = mod(div(row, dims.c), dims.x)
    zh = div(row, dims.c * dims.x)
    return dict(x=x, y=div(col, dims.zl), z=zh * dims.zl + mod(col, dims.zl), c=core)


def mesh_id(dims, p):
    row = (div(p["z"], dims.zl) * dims.x + p["x"]) * dims.c + p["c"]
    col = p["y"] * dims.zl + mod(p["z"], dims.zl)
    return (row, col)


class Plan:
    def __init__(self, dims, k, rows):
        self.dims = dims
        self.size = dict(x=dims.x, y=dims.y, z=dims.zh * dims.zl, c=dims.c)
        self.n = dims.x * dims.y * dims.zh * dims.zl * dims.c
        self.slots = 2 * self.n
        self.kt_half = k // 128 // 2
        self.rows = rows
        self.units = []
        first = 0
        for tiles, order in zip(UNIT_TILES, UNIT_ORDERS):
            self.units.append(
                dict(
                    tiles=tiles,
                    first=first,
                    order=order,
                    r1=-(-4 * tiles // 8) * 8,
                    n=[self.size[a] for a in order],
                )
            )
            first += tiles
        assert first == self.kt_half
        self.plane = dims.x * dims.y
        self.pole = self.size["z"] * dims.c


def move(me, **changes):
    return {**me, **changes}


def far_first(count):
    return sorted(range(1, count), key=lambda by: (-min(by, count - by), by))


def fused_kernel(plan, *refs):
    dims, size, n = plan.dims, plan.size, plan.n
    nu = len(plan.units)
    (pivots_in, prior_in, finished_in, pairs_in, occupied_in, out, halves) = refs[:7]
    scratch = list(refs[7:])
    take = lambda count: [scratch.pop(0) for _ in range(count)]
    (pivots, prior, finished, pairs, occupied) = take(5)
    first_out = take(nu)
    first_in = take(nu)
    gathered = take(nu)
    (partner_prior, part_out, part_in, a_out, a_in, b_out, b_in) = take(7)
    (lane, line, vector, table, masks, wheres, slots, dense, full, steps_at) = take(10)
    (load, send1, recv1, send2, recv2, send3, recv3, send_a, recv_a, send_b, recv_b,
     send_p, recv_p, send_q, recv_q, table_sem) = take(16)

    own = lax.axis_index("row") * (dims.y * dims.zl) + lax.axis_index("col")
    me = coordinates(dims, own)
    core = me["c"]
    other = move(me, c=1 - core)
    npiv = pivots.shape[1]

    def step(axis, by):
        return mod(me[axis] + by, size[axis])

    lines = []
    for axis in ("x", "y", "z"):
        for by in range(1, size[axis]):
            for c in (core, 1 - core):
                lines.append(move(me, **{axis: step(axis, by), "c": c}))
    plane_peers = []
    for bx in range(dims.x):
        for by in range(dims.y):
            if bx or by:
                far = min(bx, dims.x - bx) + min(by, dims.y - by)
                plane_peers.append((-far, move(me, x=step("x", bx), y=step("y", by))))
    plane_peers = [p for _, p in sorted(plane_peers, key=lambda item: item[0])]
    corners = []
    for bx in range(1, dims.x):
        for by in range(1, dims.y):
            corners.append(move(me, x=step("x", bx), y=step("y", by)))
    pole_peers = []
    for bz in far_first(size["z"]) + [0]:
        for c in (core, 1 - core):
            if bz or c is not core:
                pole_peers.append(move(me, z=step("z", bz), c=c))
    peers = lines + corners + [other]

    barrier = pltpu.get_barrier_semaphore()
    for p in peers:
        pl.semaphore_signal(barrier, inc=1, device_id=mesh_id(dims, p), device_id_type=MESH)

    loads = []
    for i, (src, dst) in enumerate(
        ((pivots_in, pivots), (prior_in, prior), (finished_in, finished),
         (pairs_in, pairs), (occupied_in, occupied))
    ):
        copy = pltpu.make_async_copy(src, dst, load.at[i])
        copy.start()
        loads.append(copy)

    def remote(src, dst, send, recv, p):
        copy = pltpu.make_async_remote_copy(
            src_ref=src, dst_ref=dst, send_sem=send, recv_sem=recv,
            device_id=mesh_id(dims, p), device_id_type=MESH,
        )
        copy.start()

    def wait_bytes(ref, sem):
        pltpu.make_async_copy(ref, ref, sem).wait()

    loads[0].wait()
    piv_row = jnp.broadcast_to(pivots[...], (128, npiv))
    piv_col = piv_row.astype(F32).T.astype(I32)
    here = onehot(piv_col == own * plan.rows + iota((npiv, plan.rows), 1))
    has = nn(jnp.ones((32, npiv), BF), here)
    before = onehot(iota((plan.rows, plan.rows), 0) < iota((plan.rows, plan.rows), 1))
    rank = nn(has.astype(BF), before)
    q = iota((32, plan.rows), 0)
    wanted = (mod(q, 4) - core * 2).astype(F32)
    select = jnp.where((has > 0.5) & (rank == wanted), 1.0, 0.0).astype(BF)
    loads[1].wait()
    for h in range(2):
        for u, unit in enumerate(plan.units):
            k0 = (h * plan.kt_half + unit["first"]) * 128
            rows = nn(select, prior[:, k0 : k0 + unit["tiles"] * 128])
            r1 = unit["r1"]
            part = jnp.zeros((r1, 128), F32)
            which = div(iota((r1, 128), 0), 4)
            for kt in range(unit["tiles"]):
                part = jnp.where(which == kt, rows[:r1, kt * 128 : (kt + 1) * 128], part)
            first_out[u][h] = part.astype(BF)
    for u, unit in enumerate(plan.units):
        first_in[u][me[unit["order"][0]] * dims.c + core] = first_out[u][core]

    loads[2].wait()
    r = iota((n, n), 0)
    v = coordinates(dims, iota((n, n), 1))
    spot = ((v["x"] * dims.y + v["y"]) * size["z"] + v["z"]) * dims.c + v["c"]
    a_rows = nt(onehot(r == spot), finished[...]).astype(BF)
    for i in range(plan.plane):
        a_out[i] = a_rows[i * plan.pole : (i + 1) * plan.pole]
    my_plane = me["x"] * dims.y + me["y"]
    my_pole = me["z"] * dims.c + core
    a_in[my_plane] = a_out[my_plane]

    pl.semaphore_wait(barrier, len(peers))

    for u, unit in enumerate(plan.units):
        axis = unit["order"][0]
        for by in far_first(size[axis]) + [0]:
            for c in (core, 1 - core):
                if by or c is not core:
                    remote(
                        first_out[u].at[c], first_in[u].at[me[axis] * dims.c + core],
                        send1.at[u], recv1.at[u], move(me, **{axis: step(axis, by), "c": c}),
                    )
    for p in plane_peers:
        remote(a_out.at[p["x"] * dims.y + p["y"]], a_in.at[my_plane], send_a, recv_a, p)
    half = plan.kt_half * 128
    remote(
        prior.at[:, pl.ds(pl.multiple_of((1 - core) * half, half), half)],
        partner_prior, send_p, recv_p, other,
    )

    loads[3].wait()
    flat = pairs[...].astype(F32)
    first = jnp.floor((flat + 0.5) * (1.0 / NAO)).astype(I32)
    second = pairs[...] - first * NAO
    row_block = first >> 7
    lane[...] = second & 127
    line[...] = (
        row_block * (row_block + 1) * 64 + (first & 127) * (row_block + 1) + (second >> 7)
    )
    blocks = n // 2
    total = slots.shape[0]
    last = jnp.broadcast_to(line[:, 127:128], (n, 128)) >> log2(GROUP)
    done = (mod(iota((n, 128), 0), 2) == 1) & (last <= iota((n, 128), 1))
    count = jnp.sum(jnp.where(done, 1.0, 0.0), axis=0, keepdims=True)
    leave = jnp.minimum(count, blocks - 1.0) + iota((1, 128), 1).astype(F32)
    leave_col = jnp.broadcast_to(leave, (128, 128)).T
    real = iota((128, 128), 0) < GROUPS
    rows = [leave]
    for t0 in (0, 128):
        past = real & (leave_col < (iota((128, 128), 1) + t0).astype(F32))
        rows.append(jnp.sum(jnp.where(past, 1.0, 0.0), axis=0, keepdims=True))
    which = iota((8, 128), 0)
    packed = jnp.zeros((8, 128), F32)
    for i, row in enumerate(rows):
        packed = jnp.where(which == i, jnp.broadcast_to(row, (8, 128)), packed)
    table[...] = packed.astype(I32)
    copy = pltpu.make_async_copy(table, steps_at, table_sem)
    copy.start()

    lanes = iota((128, 128), 0)
    places = iota((GROUP, 128), 0)

    def make_masks(it, carry):
        for k in range(MASK_UNROLL):
            d = it * MASK_UNROLL + k
            spread = jnp.where(lanes == lane[pl.ds(d, 1), :], 1.0, 0.0)
            masks[d] = spread.T.astype(BF)
        return carry

    def at_step(t):
        g = steps_at[1 + div(t, 128), mod(t, 128)]
        return g, jnp.clip(t - g, 0, blocks - 1)

    def make_wheres(it, carry):
        for k in range(UNROLL):
            t = it * UNROLL + k
            g, b = at_step(t)
            where = [
                onehot(places == line[pl.ds(2 * b + j, 1), :] - g * GROUP) for j in range(2)
            ]
            wheres[t] = jnp.concatenate(where, axis=1)
        return carry

    mask_steps = n // MASK_UNROLL
    lax.fori_loop(0, mask_steps // 2, make_masks, 0)

    def block_of(u, i2):
        n1, n2, n3 = plan.units[u]["n"]
        base = pl.multiple_of((me[plan.units[u]["order"][2]] * n2 + i2) * (n1 * 4), n1 * 4)
        return gathered[u].at[:, pl.ds(base, n1 * 4)]

    def pass_on(u, i2):
        unit = plan.units[u]
        a3 = unit["order"][2]
        block = block_of(u, i2)
        for by in far_first(unit["n"][2]):
            remote(block, block, send3.at[u], recv3.at[u], move(me, **{a3: step(a3, by)}))

    for u, unit in enumerate(plan.units):
        n1, n2, n3 = unit["n"]
        a1, a2, a3 = unit["order"]
        r1, tiles = unit["r1"], unit["tiles"]
        wait_bytes(first_in[u].at[pl.ds(0, n1 * dims.c - 1)], recv1.at[u])
        got = first_in[u][...].reshape(n1 * dims.c * r1, 128)
        shape = (tiles * n1 * 4, n1 * dims.c * r1)
        ro, ci = iota(shape, 0), iota(shape, 1)
        kt, slot = div(ro, n1 * 4), mod(ro, 4)
        target = (mod(div(ro, 4), n1) * dims.c + div(slot, 2)) * r1 + kt * 4 + slot
        rows = nn(onehot(ci == target), got).astype(BF)
        base = pl.multiple_of((me[a3] * n2 + me[a2]) * (n1 * 4), n1 * 4)
        for t in range(tiles):
            gathered[u][t, pl.ds(base, n1 * 4)] = rows[t * n1 * 4 : (t + 1) * n1 * 4]
        block = block_of(u, me[a2])
        for by in far_first(n2):
            remote(
                block, block, send2.at[u], recv2.at[u, me[a2]], move(me, **{a2: step(a2, by)})
            )
        pass_on(u, me[a2])

    wait_bytes(a_in.at[pl.ds(0, plan.plane - 1)], recv_a)
    mixed = a_in[...].reshape(n, plan.rows)
    source = mod(r, plan.plane) * plan.pole + div(r, plan.plane)
    b_rows = nn(onehot(iota((n, n), 1) == source), mixed).astype(BF)
    for i in range(plan.pole):
        b_out[i] = b_rows[i * plan.plane : (i + 1) * plan.plane]
    b_in[my_pole] = b_out[my_pole]
    for p in pole_peers:
        remote(b_out.at[p["z"] * dims.c + p["c"]], b_in.at[my_pole], send_b, recv_b, p)

    copy.wait()
    lax.fori_loop(0, total // UNROLL, make_wheres, 0)

    for u, unit in enumerate(plan.units):
        a2 = unit["order"][1]
        for by in reversed(far_first(unit["n"][1])):
            i2 = step(a2, by)
            wait_bytes(block_of(u, i2), recv2.at[u, i2])
            pass_on(u, i2)

    lax.fori_loop(mask_steps // 2, mask_steps, make_masks, 0)

    wait_bytes(b_in.at[pl.ds(0, plan.pole - 1)], recv_b)
    mixed = b_in[...].reshape(n, plan.rows)
    w = coordinates(dims, r)
    source = (w["z"] * dims.c + w["c"]) * plan.plane + w["x"] * dims.y + w["y"]
    vector[...] = nn(onehot(iota((n, n), 1) == source), mixed)

    def scatter(it, carry):
        acc, before = carry
        for k in range(UNROLL):
            t = it * UNROLL + k
            g, b = at_step(t)
            scale = [
                jnp.broadcast_to(vector[pl.ds(2 * b + j, 1), :], (GROUP, 128)).astype(BF)
                for j in range(2)
            ]
            left = wheres[t] * jnp.concatenate(scale, axis=1)
            right = masks[pl.ds(2 * b, 2)].reshape(BLOCK, 128)
            acc = jnp.where(g == before, acc, 0.0) + nn(left, right)
            slots[t] = acc
            before = g
        return acc, before

    lax.fori_loop(
        0, total // UNROLL, scatter, (jnp.zeros((GROUP, 128), F32), jnp.int32(-1))
    )
    for g in range(GROUPS):
        dense[g * GROUP : (g + 1) * GROUP, :] = slots[jnp.clip(steps_at[0, g], 0, total - 1)]

    same = iota((128, 128), 0) == iota((128, 128), 1)
    for big in range(7):
        height = min(128, NAO - big * 128)
        base = 64 * big * (big + 1)
        for c in range(big + 1):
            tile = dense[pl.ds(base + c, height, stride=big + 1), :]
            if height < 128:
                tile = jnp.concatenate([tile, jnp.zeros((128 - height, 128), F32)], axis=0)
            flip = tile.T
            if c == big:
                tile = jnp.where(same, tile, tile + flip)
            else:
                full[c * 128 : (c + 1) * 128, big * 128 : (big + 1) * 128] = flip.astype(BF)
            full[big * 128 : (big + 1) * 128, c * 128 : (c + 1) * 128] = tile.astype(BF)
    loads[4].wait()
    for big in range(7):
        height = min(128, NAO - big * 128)
        rows = nn(full[big * 128 : (big + 1) * 128, :NAO], occupied[...])
        halves[big * 128 : big * 128 + height, :] = rows[:height]

    lower = []
    for j0 in range(0, npiv, 128):
        pr = piv_row[:1, j0 : j0 + 128] if npiv >= 128 else piv_row[:1]
        pc = piv_col[:, : pr.shape[1]]
        lower.append(onehot((div(pc, plan.rows) == div(pr, plan.rows)) & (pr < pc)))
    lower = jnp.concatenate(lower, axis=1)
    place = nn(lower, jnp.ones((npiv, 128), BF)).astype(I32)
    o = coordinates(dims, div(piv_col, plan.rows))

    wait_bytes(partner_prior, recv_p)
    mine = jnp.zeros((plan.rows, npiv), F32)
    theirs = jnp.zeros((plan.rows, npiv), F32)
    for u, unit in enumerate(plan.units):
        n1, n2, n3 = unit["n"]
        a1, a2, a3 = unit["order"]
        tiles = unit["tiles"]
        wait_bytes(gathered[u].at[:, pl.ds(0, n2 * n1 * 4 * (n3 - 1))], recv3.at[u])
        at = ((o[a3] * n2 + o[a2]) * n1 + o[a1]) * 4 + o["c"] * 2 + place
        pick = jnp.concatenate(
            [onehot(iota((npiv, 128), 1) + s == at) for s in range(0, plan.slots, 128)], axis=1
        )
        pick = pick[:, : plan.slots]
        rows = jnp.concatenate(
            [nn(pick, gathered[u][t]).astype(BF) for t in range(tiles)], axis=1
        )
        k0 = unit["first"] * 128
        at_k = pl.multiple_of(core * half + k0, 128)
        mine += nt(prior[:, pl.ds(at_k, tiles * 128)], rows)
        theirs += nt(partner_prior[:, k0 : k0 + tiles * 128], rows)
    part_out[...] = theirs
    remote(part_out, part_in, send_q, recv_q, other)

    for u, unit in enumerate(plan.units):
        n1, n2, n3 = unit["n"]
        wait_bytes(first_in[u].at[pl.ds(0, n1 * dims.c - 1)], send1.at[u])
        wait_bytes(gathered[u].at[:, pl.ds(0, n1 * 4 * (n2 - 1))], send2.at[u])
        wait_bytes(gathered[u].at[:, pl.ds(0, n2 * n1 * 4 * (n3 - 1))], send3.at[u])
    wait_bytes(a_in.at[pl.ds(0, plan.plane - 1)], send_a)
    wait_bytes(b_in.at[pl.ds(0, plan.pole - 1)], send_b)
    wait_bytes(partner_prior, send_p)
    wait_bytes(part_in, recv_q)
    wait_bytes(part_out, send_q)
    out[...] = mine + part_in[...]


def run_kernel(plan, pivots, prior, finished, pairs, occupied):
    npiv = pivots.shape[0]
    vmem = pl.BlockSpec(memory_space=pltpu.VMEM)
    anywhere = pl.BlockSpec(memory_space=pl.ANY)
    dma = pltpu.SemaphoreType.DMA
    nu = len(plan.units)
    n, rows = plan.n, plan.rows
    blocks = n // 2
    total = -(-(GROUPS + blocks - 1) // UNROLL) * UNROLL
    scratch = [
        pltpu.VMEM((1, npiv), I32),
        pltpu.VMEM(prior.shape, BF),
        pltpu.VMEM(finished.shape, BF),
        pltpu.VMEM((n, rows), I32),
        pltpu.VMEM(occupied.shape, BF),
    ]
    scratch += [pltpu.VMEM((2, u["r1"], 128), BF) for u in plan.units]
    scratch += [pltpu.VMEM((u["n"][0] * plan.dims.c, u["r1"], 128), BF) for u in plan.units]
    scratch += [pltpu.VMEM((u["tiles"], plan.slots, 128), BF) for u in plan.units]
    scratch += [
        pltpu.VMEM((rows, plan.kt_half * 128), BF),
        pltpu.VMEM((rows, npiv), F32),
        pltpu.VMEM((rows, npiv), F32),
        pltpu.VMEM((plan.plane, plan.pole, rows), BF),
        pltpu.VMEM((plan.plane, plan.pole, rows), BF),
        pltpu.VMEM((plan.pole, plan.plane, rows), BF),
        pltpu.VMEM((plan.pole, plan.plane, rows), BF),
        pltpu.VMEM((n, 128), I32),
        pltpu.VMEM((n, 128), I32),
        pltpu.VMEM((n, 128), F32),
        pltpu.VMEM((8, 128), I32),
        pltpu.VMEM((n, 128, 128), BF),
        pltpu.VMEM((total, GROUP, BLOCK), BF),
        pltpu.VMEM((total, GROUP, 128), F32),
        pltpu.VMEM((GROUPS * GROUP, 128), F32),
        pltpu.VMEM((896, 896), BF),
        pltpu.SMEM((8, 128), I32),
    ]
    scratch += [dma((5,)), dma((nu,)), dma((nu,)), dma((nu,)), dma((nu, 8))]
    scratch += [dma((nu,)), dma((nu,))] + [dma] * 9
    return pl.pallas_call(
        functools.partial(fused_kernel, plan),
        out_shape=(
            jax.ShapeDtypeStruct((rows, npiv), F32),
            jax.ShapeDtypeStruct((NAO, occupied.shape[1]), F32),
        ),
        in_specs=[anywhere] * 5,
        out_specs=(vmem, vmem),
        scratch_shapes=scratch,
        compiler_params=pltpu.CompilerParams(
            collective_id=0, has_side_effects=True, vmem_limit_bytes=34 * 1024 * 1024
        ),
        name="fused",
    )(pivots.reshape(1, npiv), prior, finished, pairs.reshape(n, rows), occupied)


def per_device(dims, pivots, panel, prior, finished, pairs, occupied):
    plan = Plan(dims, prior.shape[1], prior.shape[0])
    product, flipped = run_kernel(plan, pivots, prior, finished, pairs, occupied)
    return panel - product, flipped.T[None]


def build(mesh, dims):
    return jax.shard_map(
        functools.partial(per_device, dims),
        mesh=mesh,
        in_specs=(
            P(),
            P(("row", "col"), None),
            P(("row", "col"), None),
            P(("row", "col"), None),
            P(),
            P(),
        ),
        out_specs=(P(("row", "col"), None), P(("row", "col"), None, None)),
        check_vma=False,
    )


def solution(mesh):
    return build(mesh, FULL)
```

```python
import functools
import math
from collections import namedtuple

import jax
import jax.numpy as jnp
from jax import lax
from jax.experimental import pallas as pl
from jax.experimental.pallas import tpu as pltpu
from jax.sharding import PartitionSpec as P

MESH = pl.DeviceIdType.MESH
BF, F32, I32 = jnp.bfloat16, jnp.float32, jnp.int32
Dims = namedtuple("Dims", ("x", "y", "zh", "zl", "c"))
FULL = Dims(4, 4, 4, 2, 2)

NAO = 800
GROUP = 64
BLOCK = 256
GROUPS = 46
UNROLL = 22
WHERE_UNROLL = 8
MASK_UNROLL = 16

UNIT_TILES = (2, 5, 5)
UNIT_ORDERS = (("x", "y", "z"), ("y", "z", "x"), ("z", "x", "y"))


def nt(a, b):
    return lax.dot_general(a, b, (((1,), (1,)), ((), ())), preferred_element_type=F32)


def nn(a, b):
    return lax.dot_general(a, b, (((1,), (0,)), ((), ())), preferred_element_type=F32)


def iota(shape, dim):
    return lax.broadcasted_iota(I32, shape, dim)


def log2(n):
    assert n & (n - 1) == 0
    return n.bit_length() - 1


def mod(v, n):
    return v & (n - 1)


def div(v, n):
    return v >> log2(n)


def onehot(cond):
    return jnp.where(cond, 1.0, 0.0).astype(BF)


def coordinates(dims, device):
    col = mod(device, dims.y * dims.zl)
    row = div(device, dims.y * dims.zl)
    core = mod(row, dims.c)
    x = mod(div(row, dims.c), dims.x)
    zh = div(row, dims.c * dims.x)
    return dict(x=x, y=div(col, dims.zl), z=zh * dims.zl + mod(col, dims.zl), c=core)


def mesh_id(dims, p):
    row = (div(p["z"], dims.zl) * dims.x + p["x"]) * dims.c + p["c"]
    col = p["y"] * dims.zl + mod(p["z"], dims.zl)
    return (row, col)


class Plan:
    def __init__(self, dims, k, rows):
        self.dims = dims
        self.size = dict(x=dims.x, y=dims.y, z=dims.zh * dims.zl, c=dims.c)
        self.n = dims.x * dims.y * dims.zh * dims.zl * dims.c
        self.slots = 2 * self.n
        self.kt_half = k // 128 // 2
        self.rows = rows
        self.units = []
        first = 0
        for tiles, order in zip(UNIT_TILES, UNIT_ORDERS):
            self.units.append(
                dict(
                    tiles=tiles,
                    first=first,
                    order=order,
                    r1=-(-4 * tiles // 8) * 8,
                    n=[self.size[a] for a in order],
                )
            )
            first += tiles
        assert first == self.kt_half
        self.plane = dims.x * dims.y
        self.pole = self.size["z"] * dims.c


def move(me, **changes):
    return {**me, **changes}


def steps_of(blocks):
    both = UNROLL * WHERE_UNROLL // math.gcd(UNROLL, WHERE_UNROLL)
    return -(-(GROUPS + blocks - 1) // both) * both


def far_first(count):
    return sorted(range(1, count), key=lambda by: (-min(by, count - by), by))


def fused_kernel(plan, *refs):
    dims, size, n = plan.dims, plan.size, plan.n
    nu = len(plan.units)
    (pivots_in, prior_in, finished_in, pairs_in, occupied_in, out, halves) = refs[:7]
    scratch = list(refs[7:])
    take = lambda count: [scratch.pop(0) for _ in range(count)]
    (pivots, prior, finished, pairs, occupied) = take(5)
    first_out = take(nu)
    first_in = take(nu)
    gathered = take(nu)
    (partner_prior, part_out, part_in, a_out, a_in, b_out, b_in) = take(7)
    (lane, line, vector, table, masks, wheres, slots, dense, full, picks, steps_at) = take(11)
    (load, send1, recv1, send2, recv2, send3, recv3, send_a, recv_a, send_b, recv_b,
     send_p, recv_p, send_q, recv_q, table_sem) = take(16)

    own = lax.axis_index("row") * (dims.y * dims.zl) + lax.axis_index("col")
    me = coordinates(dims, own)
    core = me["c"]
    other = move(me, c=1 - core)
    npiv = pivots.shape[1]

    def step(axis, by):
        return mod(me[axis] + by, size[axis])

    lines = []
    for axis in ("x", "y", "z"):
        for by in range(1, size[axis]):
            for c in (core, 1 - core):
                lines.append(move(me, **{axis: step(axis, by), "c": c}))
    plane_peers = []
    for bx in range(dims.x):
        for by in range(dims.y):
            if bx or by:
                far = min(bx, dims.x - bx) + min(by, dims.y - by)
                plane_peers.append((-far, move(me, x=step("x", bx), y=step("y", by))))
    plane_peers = [p for _, p in sorted(plane_peers, key=lambda item: item[0])]
    corners = []
    for bx in range(1, dims.x):
        for by in range(1, dims.y):
            corners.append(move(me, x=step("x", bx), y=step("y", by)))
    pole_peers = []
    for bz in far_first(size["z"]) + [0]:
        for c in (core, 1 - core):
            if bz or c is not core:
                pole_peers.append(move(me, z=step("z", bz), c=c))
    peers = lines + corners + [other]

    barrier = pltpu.get_barrier_semaphore()
    for p in peers:
        pl.semaphore_signal(barrier, inc=1, device_id=mesh_id(dims, p), device_id_type=MESH)

    loads = []
    for i, (src, dst) in enumerate(
        ((pivots_in, pivots), (prior_in, prior), (finished_in, finished),
         (pairs_in, pairs), (occupied_in, occupied))
    ):
        copy = pltpu.make_async_copy(src, dst, load.at[i])
        copy.start()
        loads.append(copy)

    def remote(src, dst, send, recv, p):
        copy = pltpu.make_async_remote_copy(
            src_ref=src, dst_ref=dst, send_sem=send, recv_sem=recv,
            device_id=mesh_id(dims, p), device_id_type=MESH,
        )
        copy.start()

    def wait_bytes(ref, sem):
        pltpu.make_async_copy(ref, ref, sem).wait()

    loads[0].wait()
    piv_row = jnp.broadcast_to(pivots[...], (128, npiv))
    piv_col = piv_row.astype(F32).T.astype(I32)
    here = onehot(piv_col == own * plan.rows + iota((npiv, plan.rows), 1))
    has = nn(jnp.ones((32, npiv), BF), here)
    before = onehot(iota((plan.rows, plan.rows), 0) < iota((plan.rows, plan.rows), 1))
    rank = nn(has.astype(BF), before)
    q = iota((32, plan.rows), 0)
    wanted = (mod(q, 4) - core * 2).astype(F32)
    select = jnp.where((has > 0.5) & (rank == wanted), 1.0, 0.0).astype(BF)
    loads[1].wait()
    for h in range(2):
        for u, unit in enumerate(plan.units):
            k0 = (h * plan.kt_half + unit["first"]) * 128
            rows = nn(select, prior[:, k0 : k0 + unit["tiles"] * 128])
            r1 = unit["r1"]
            part = jnp.zeros((r1, 128), F32)
            which = div(iota((r1, 128), 0), 4)
            for kt in range(unit["tiles"]):
                part = jnp.where(which == kt, rows[:r1, kt * 128 : (kt + 1) * 128], part)
            first_out[u][h] = part.astype(BF)
    for u, unit in enumerate(plan.units):
        first_in[u][me[unit["order"][0]] * dims.c + core] = first_out[u][core]

    loads[2].wait()
    r = iota((n, n), 0)
    v = coordinates(dims, iota((n, n), 1))
    spot = ((v["x"] * dims.y + v["y"]) * size["z"] + v["z"]) * dims.c + v["c"]
    a_rows = nt(onehot(r == spot), finished[...]).astype(BF)
    for i in range(plan.plane):
        a_out[i] = a_rows[i * plan.pole : (i + 1) * plan.pole]
    my_plane = me["x"] * dims.y + me["y"]
    my_pole = me["z"] * dims.c + core
    a_in[my_plane] = a_out[my_plane]

    pl.semaphore_wait(barrier, len(peers))

    for u, unit in enumerate(plan.units):
        axis = unit["order"][0]
        for by in far_first(size[axis]) + [0]:
            for c in (core, 1 - core):
                if by or c is not core:
                    remote(
                        first_out[u].at[c], first_in[u].at[me[axis] * dims.c + core],
                        send1.at[u], recv1.at[u], move(me, **{axis: step(axis, by), "c": c}),
                    )
    for p in plane_peers:
        remote(a_out.at[p["x"] * dims.y + p["y"]], a_in.at[my_plane], send_a, recv_a, p)
    half = plan.kt_half * 128
    remote(
        prior.at[:, pl.ds(pl.multiple_of((1 - core) * half, half), half)],
        partner_prior, send_p, recv_p, other,
    )

    loads[3].wait()
    flat = pairs[...].astype(F32)
    first = jnp.floor((flat + 0.5) * (1.0 / NAO)).astype(I32)
    second = pairs[...] - first * NAO
    row_block = first >> 7
    lane[...] = second & 127
    line[...] = (
        row_block * (row_block + 1) * 64 + (first & 127) * (row_block + 1) + (second >> 7)
    )
    blocks = n // 2
    total = slots.shape[0]
    last = jnp.broadcast_to(line[:, 127:128], (n, 128)) >> log2(GROUP)
    done = (mod(iota((n, 128), 0), 2) == 1) & (last <= iota((n, 128), 1))
    count = jnp.sum(jnp.where(done, 1.0, 0.0), axis=0, keepdims=True)
    leave = jnp.minimum(count, blocks - 1.0) + iota((1, 128), 1).astype(F32)
    leave_col = jnp.broadcast_to(leave, (128, 128)).T
    real = iota((128, 128), 0) < GROUPS
    rows = [leave]
    for t0 in (0, 128):
        past = real & (leave_col < (iota((128, 128), 1) + t0).astype(F32))
        rows.append(jnp.sum(jnp.where(past, 1.0, 0.0), axis=0, keepdims=True))
    which = iota((8, 128), 0)
    packed = jnp.zeros((8, 128), F32)
    for i, row in enumerate(rows):
        packed = jnp.where(which == i, jnp.broadcast_to(row, (8, 128)), packed)
    table[...] = packed.astype(I32)
    copy = pltpu.make_async_copy(table, steps_at, table_sem)
    copy.start()

    lanes = iota((128, 128), 0)
    places = iota((GROUP, 128), 0)

    def make_masks(it, carry):
        for k in range(MASK_UNROLL):
            d = it * MASK_UNROLL + k
            masks[d] = onehot(lanes == lane[pl.ds(d, 1), :]).T
        return carry

    def at_step(t):
        g = steps_at[1 + div(t, 128), mod(t, 128)]
        return g, jnp.clip(t - g, 0, blocks - 1)

    def make_wheres(it, carry):
        for k in range(WHERE_UNROLL):
            t = it * WHERE_UNROLL + k
            g, b = at_step(t)
            where = [
                onehot(places == line[pl.ds(2 * b + j, 1), :] - g * GROUP) for j in range(2)
            ]
            wheres[t] = jnp.concatenate(where, axis=1)
        return carry

    mask_steps = max(1, n // MASK_UNROLL)
    lax.fori_loop(0, mask_steps // 2, make_masks, 0)

    def block_of(u, i2):
        n1, n2, n3 = plan.units[u]["n"]
        base = pl.multiple_of((me[plan.units[u]["order"][2]] * n2 + i2) * (n1 * 4), n1 * 4)
        return gathered[u].at[:, pl.ds(base, n1 * 4)]

    def pass_on(u, i2):
        unit = plan.units[u]
        a3 = unit["order"][2]
        block = block_of(u, i2)
        for by in far_first(unit["n"][2]):
            remote(block, block, send3.at[u], recv3.at[u], move(me, **{a3: step(a3, by)}))

    for u, unit in enumerate(plan.units):
        n1, n2, n3 = unit["n"]
        a1, a2, a3 = unit["order"]
        r1, tiles = unit["r1"], unit["tiles"]
        wait_bytes(first_in[u].at[pl.ds(0, n1 * dims.c - 1)], recv1.at[u])
        got = first_in[u][...].reshape(n1 * dims.c * r1, 128)
        shape = (tiles * n1 * 4, n1 * dims.c * r1)
        ro, ci = iota(shape, 0), iota(shape, 1)
        kt, slot = div(ro, n1 * 4), mod(ro, 4)
        target = (mod(div(ro, 4), n1) * dims.c + div(slot, 2)) * r1 + kt * 4 + slot
        rows = nn(onehot(ci == target), got).astype(BF)
        base = pl.multiple_of((me[a3] * n2 + me[a2]) * (n1 * 4), n1 * 4)
        for t in range(tiles):
            gathered[u][t, pl.ds(base, n1 * 4)] = rows[t * n1 * 4 : (t + 1) * n1 * 4]
        block = block_of(u, me[a2])
        for by in far_first(n2):
            remote(
                block, block, send2.at[u], recv2.at[u, me[a2]], move(me, **{a2: step(a2, by)})
            )
        pass_on(u, me[a2])

    wait_bytes(a_in.at[pl.ds(0, plan.plane - 1)], recv_a)
    mixed = a_in[...].reshape(n, plan.rows)
    source = mod(r, plan.plane) * plan.pole + div(r, plan.plane)
    b_rows = nn(onehot(iota((n, n), 1) == source), mixed).astype(BF)
    for i in range(plan.pole):
        b_out[i] = b_rows[i * plan.plane : (i + 1) * plan.plane]
    b_in[my_pole] = b_out[my_pole]
    for p in pole_peers:
        remote(b_out.at[p["z"] * dims.c + p["c"]], b_in.at[my_pole], send_b, recv_b, p)

    copy.wait()
    lax.fori_loop(0, total // WHERE_UNROLL, make_wheres, 0)

    def pass_on_arrivals(u):
        unit = plan.units[u]
        a2 = unit["order"][1]
        for by in reversed(far_first(unit["n"][1])):
            i2 = step(a2, by)
            wait_bytes(block_of(u, i2), recv2.at[u, i2])
            pass_on(u, i2)

    pass_on_arrivals(0)
    pass_on_arrivals(2)
    lax.fori_loop(mask_steps // 2, mask_steps, make_masks, 0)

    lower = []
    for j0 in range(0, npiv, 128):
        pr = piv_row[:1, j0 : j0 + 128] if npiv >= 128 else piv_row[:1]
        pc = piv_col[:, : pr.shape[1]]
        lower.append(onehot((div(pc, plan.rows) == div(pr, plan.rows)) & (pr < pc)))
    lower = jnp.concatenate(lower, axis=1)
    place = nn(lower, jnp.ones((npiv, 128), BF)).astype(I32)
    o = coordinates(dims, div(piv_col, plan.rows))
    for u, unit in enumerate(plan.units):
        n1, n2, n3 = unit["n"]
        a1, a2, a3 = unit["order"]
        at = ((o[a3] * n2 + o[a2]) * n1 + o[a1]) * 4 + o["c"] * 2 + place
        pick = jnp.concatenate(
            [onehot(iota((npiv, 128), 1) + s == at) for s in range(0, plan.slots, 128)], axis=1
        )
        picks[u] = pick[:, : plan.slots]
    pass_on_arrivals(1)

    wait_bytes(b_in.at[pl.ds(0, plan.pole - 1)], recv_b)
    mixed = b_in[...].reshape(n, plan.rows)
    w = coordinates(dims, r)
    source = (w["z"] * dims.c + w["c"]) * plan.plane + w["x"] * dims.y + w["y"]
    vector[...] = nn(onehot(iota((n, n), 1) == source), mixed)

    def scatter(it, carry):
        acc, before = carry
        for k in range(UNROLL):
            t = it * UNROLL + k
            g, b = at_step(t)
            scale = [
                jnp.broadcast_to(vector[pl.ds(2 * b + j, 1), :], (GROUP, 128)).astype(BF)
                for j in range(2)
            ]
            left = wheres[t] * jnp.concatenate(scale, axis=1)
            right = masks[pl.ds(2 * b, 2)].reshape(BLOCK, 128)
            acc = jnp.where(g == before, acc, 0.0) + nn(left, right)
            slots[t] = acc
            before = g
        return acc, before

    lax.fori_loop(
        0, total // UNROLL, scatter, (jnp.zeros((GROUP, 128), F32), jnp.int32(-1))
    )
    for g in range(GROUPS):
        dense[g * GROUP : (g + 1) * GROUP, :] = slots[jnp.clip(steps_at[0, g], 0, total - 1)]

    same = iota((128, 128), 0) == iota((128, 128), 1)
    for big in range(7):
        height = min(128, NAO - big * 128)
        base = 64 * big * (big + 1)
        for c in range(big + 1):
            tile = dense[pl.ds(base + c, height, stride=big + 1), :]
            if height < 128:
                tile = jnp.concatenate([tile, jnp.zeros((128 - height, 128), F32)], axis=0)
            flip = tile.T
            if c == big:
                tile = jnp.where(same, tile, tile + flip)
            else:
                full[c * 128 : (c + 1) * 128, big * 128 : (big + 1) * 128] = flip.astype(BF)
            full[big * 128 : (big + 1) * 128, c * 128 : (c + 1) * 128] = tile.astype(BF)
    loads[4].wait()
    for big in range(7):
        height = min(128, NAO - big * 128)
        rows = nn(full[big * 128 : (big + 1) * 128, :NAO], occupied[...])
        halves[big * 128 : big * 128 + height, :] = rows[:height]

    wait_bytes(partner_prior, recv_p)
    theirs = jnp.zeros((plan.rows, npiv), F32)
    chosen = []
    for u in (0, 2, 1):
        unit = plan.units[u]
        n1, n2, n3 = unit["n"]
        tiles = unit["tiles"]
        wait_bytes(gathered[u].at[:, pl.ds(0, n2 * n1 * 4 * (n3 - 1))], recv3.at[u])
        rows = jnp.concatenate(
            [nn(picks[u], gathered[u][t]).astype(BF) for t in range(tiles)], axis=1
        )
        chosen.append((unit, rows))
        k0 = unit["first"] * 128
        theirs += nt(partner_prior[:, k0 : k0 + tiles * 128], rows)
    part_out[...] = theirs
    remote(part_out, part_in, send_q, recv_q, other)
    mine = jnp.zeros((plan.rows, npiv), F32)
    for unit, rows in chosen:
        at_k = pl.multiple_of(core * half + unit["first"] * 128, 128)
        mine += nt(prior[:, pl.ds(at_k, unit["tiles"] * 128)], rows)

    for u, unit in enumerate(plan.units):
        n1, n2, n3 = unit["n"]
        wait_bytes(first_in[u].at[pl.ds(0, n1 * dims.c - 1)], send1.at[u])
        wait_bytes(gathered[u].at[:, pl.ds(0, n1 * 4 * (n2 - 1))], send2.at[u])
        wait_bytes(gathered[u].at[:, pl.ds(0, n2 * n1 * 4 * (n3 - 1))], send3.at[u])
    wait_bytes(a_in.at[pl.ds(0, plan.plane - 1)], send_a)
    wait_bytes(b_in.at[pl.ds(0, plan.pole - 1)], send_b)
    wait_bytes(partner_prior, send_p)
    wait_bytes(part_in, recv_q)
    wait_bytes(part_out, send_q)
    out[...] = mine + part_in[...]


def run_kernel(plan, pivots, prior, finished, pairs, occupied):
    npiv = pivots.shape[0]
    vmem = pl.BlockSpec(memory_space=pltpu.VMEM)
    anywhere = pl.BlockSpec(memory_space=pl.ANY)
    dma = pltpu.SemaphoreType.DMA
    nu = len(plan.units)
    n, rows = plan.n, plan.rows
    blocks = n // 2
    total = steps_of(blocks)
    scratch = [
        pltpu.VMEM((1, npiv), I32),
        pltpu.VMEM(prior.shape, BF),
        pltpu.VMEM(finished.shape, BF),
        pltpu.VMEM((n, rows), I32),
        pltpu.VMEM(occupied.shape, BF),
    ]
    scratch += [pltpu.VMEM((2, u["r1"], 128), BF) for u in plan.units]
    scratch += [pltpu.VMEM((u["n"][0] * plan.dims.c, u["r1"], 128), BF) for u in plan.units]
    scratch += [pltpu.VMEM((u["tiles"], plan.slots, 128), BF) for u in plan.units]
    scratch += [
        pltpu.VMEM((rows, plan.kt_half * 128), BF),
        pltpu.VMEM((rows, npiv), F32),
        pltpu.VMEM((rows, npiv), F32),
        pltpu.VMEM((plan.plane, plan.pole, rows), BF),
        pltpu.VMEM((plan.plane, plan.pole, rows), BF),
        pltpu.VMEM((plan.pole, plan.plane, rows), BF),
        pltpu.VMEM((plan.pole, plan.plane, rows), BF),
        pltpu.VMEM((n, 128), I32),
        pltpu.VMEM((n, 128), I32),
        pltpu.VMEM((n, 128), F32),
        pltpu.VMEM((8, 128), I32),
        pltpu.VMEM((n, 128, 128), BF),
        pltpu.VMEM((total, GROUP, BLOCK), BF),
        pltpu.VMEM((total, GROUP, 128), F32),
        pltpu.VMEM((GROUPS * GROUP, 128), F32),
        pltpu.VMEM((896, 896), BF),
        pltpu.VMEM((nu, npiv, plan.slots), BF),
        pltpu.SMEM((8, 128), I32),
    ]
    scratch += [dma((5,)), dma((nu,)), dma((nu,)), dma((nu,)), dma((nu, 8))]
    scratch += [dma((nu,)), dma((nu,))] + [dma] * 9
    return pl.pallas_call(
        functools.partial(fused_kernel, plan),
        out_shape=(
            pltpu.VMEM((rows, npiv), F32),
            pltpu.VMEM((NAO, occupied.shape[1]), F32),
        ),
        in_specs=[anywhere] * 5,
        out_specs=(vmem, vmem),
        scratch_shapes=scratch,
        compiler_params=pltpu.CompilerParams(
            collective_id=0, has_side_effects=True, vmem_limit_bytes=56 * 1024 * 1024
        ),
        name="fused",
    )(pivots.reshape(1, npiv), prior, finished, pairs.reshape(n, rows), occupied)


def finish_kernel(panel, product, flipped, updated, halves, result, sems):
    first = pltpu.make_async_copy(flipped, halves, sems.at[0])
    first.start()
    result[...] = panel[...] - product[...]
    second = pltpu.make_async_copy(result, updated, sems.at[1])
    second.start()
    first.wait()
    second.wait()


def finish(panel, product, flipped):
    vmem = pl.BlockSpec(memory_space=pltpu.VMEM)
    hbm = pl.BlockSpec(memory_space=pltpu.HBM)
    return pl.pallas_call(
        finish_kernel,
        out_shape=(pltpu.HBM(panel.shape, F32), pltpu.HBM(flipped.shape, F32)),
        in_specs=[vmem] * 3,
        out_specs=(hbm, hbm),
        scratch_shapes=[pltpu.VMEM(panel.shape, F32), pltpu.SemaphoreType.DMA((2,))],
        compiler_params=pltpu.CompilerParams(vmem_limit_bytes=4 * 1024 * 1024),
        name="finish",
    )(panel, product, flipped)


def per_device(dims, pivots, panel, prior, finished, pairs, occupied):
    plan = Plan(dims, prior.shape[1], prior.shape[0])
    product, flipped = run_kernel(plan, pivots, prior, finished, pairs, occupied)
    updated, flipped = finish(panel, product, flipped)
    return updated, flipped.T[None]


def build(mesh, dims):
    return jax.shard_map(
        functools.partial(per_device, dims),
        mesh=mesh,
        in_specs=(
            P(),
            P(("row", "col"), None),
            P(("row", "col"), None),
            P(("row", "col"), None),
            P(),
            P(),
        ),
        out_specs=(P(("row", "col"), None), P(("row", "col"), None, None)),
        check_vma=False,
    )


def solution(mesh):
    return build(mesh, FULL)
```

```python
import functools
import math
from collections import namedtuple

import jax
import jax.numpy as jnp
from jax import lax
from jax.experimental import pallas as pl
from jax.experimental.pallas import tpu as pltpu
from jax.sharding import PartitionSpec as P

MESH = pl.DeviceIdType.MESH
BF, F32, I32 = jnp.bfloat16, jnp.float32, jnp.int32
Dims = namedtuple("Dims", ("x", "y", "zh", "zl", "c"))
FULL = Dims(4, 4, 4, 2, 2)

NAO = 800
GROUP = 64
BLOCK = 256
GROUPS = 46
UNROLL = 22
WHERE_UNROLL = 8
MASK_UNROLL = 16

UNIT_TILES = (2, 4, 6)
UNIT_ORDERS = (("x", "y", "z"), ("y", "z", "x"), ("z", "x", "y"))


def nt(a, b):
    return lax.dot_general(a, b, (((1,), (1,)), ((), ())), preferred_element_type=F32)


def nn(a, b):
    return lax.dot_general(a, b, (((1,), (0,)), ((), ())), preferred_element_type=F32)


def iota(shape, dim):
    return lax.broadcasted_iota(I32, shape, dim)


def log2(n):
    assert n & (n - 1) == 0
    return n.bit_length() - 1


def mod(v, n):
    return v & (n - 1)


def div(v, n):
    return v >> log2(n)


def onehot(cond):
    return jnp.where(cond, 1.0, 0.0).astype(BF)


def coordinates(dims, device):
    col = mod(device, dims.y * dims.zl)
    row = div(device, dims.y * dims.zl)
    core = mod(row, dims.c)
    x = mod(div(row, dims.c), dims.x)
    zh = div(row, dims.c * dims.x)
    return dict(x=x, y=div(col, dims.zl), z=zh * dims.zl + mod(col, dims.zl), c=core)


def mesh_id(dims, p):
    row = (div(p["z"], dims.zl) * dims.x + p["x"]) * dims.c + p["c"]
    col = p["y"] * dims.zl + mod(p["z"], dims.zl)
    return (row, col)


class Plan:
    def __init__(self, dims, k, rows):
        self.dims = dims
        self.size = dict(x=dims.x, y=dims.y, z=dims.zh * dims.zl, c=dims.c)
        self.n = dims.x * dims.y * dims.zh * dims.zl * dims.c
        self.slots = 2 * self.n
        self.kt_half = k // 128 // 2
        self.rows = rows
        self.units = []
        first = 0
        for tiles, order in zip(UNIT_TILES, UNIT_ORDERS):
            self.units.append(
                dict(
                    tiles=tiles,
                    first=first,
                    order=order,
                    r1=-(-4 * tiles // 8) * 8,
                    n=[self.size[a] for a in order],
                )
            )
            first += tiles
        assert first == self.kt_half
        self.plane = dims.x * dims.y
        self.pole = self.size["z"] * dims.c


def move(me, **changes):
    return {**me, **changes}


def steps_of(blocks):
    both = UNROLL * WHERE_UNROLL // math.gcd(UNROLL, WHERE_UNROLL)
    return -(-(GROUPS + blocks - 1) // both) * both


def far_first(count):
    return sorted(range(1, count), key=lambda by: (-min(by, count - by), by))


def fused_kernel(plan, *refs):
    dims, size, n = plan.dims, plan.size, plan.n
    nu = len(plan.units)
    (pivots_in, prior_in, finished_in, pairs_in, occupied_in, out, halves) = refs[:7]
    scratch = list(refs[7:])
    take = lambda count: [scratch.pop(0) for _ in range(count)]
    (pivots, prior, finished, pairs, occupied) = take(5)
    first_out = take(nu)
    first_in = take(nu)
    gathered = take(nu)
    (partner_prior, part_out, part_in, a_out, a_in, b_out, b_in) = take(7)
    (lane, line, vector, table, masks, wheres, slots, dense, full, picks, steps_at) = take(11)
    (load, send1, recv1, send2, recv2, send3, recv3, send_a, recv_a, send_b, recv_b,
     send_p, recv_p, send_q, recv_q, table_sem) = take(16)

    own = lax.axis_index("row") * (dims.y * dims.zl) + lax.axis_index("col")
    me = coordinates(dims, own)
    core = me["c"]
    other = move(me, c=1 - core)
    npiv = pivots.shape[1]

    def step(axis, by):
        return mod(me[axis] + by, size[axis])

    lines = []
    for axis in ("x", "y", "z"):
        for by in range(1, size[axis]):
            for c in (core, 1 - core):
                lines.append(move(me, **{axis: step(axis, by), "c": c}))
    plane_peers = []
    for bx in range(dims.x):
        for by in range(dims.y):
            if bx or by:
                far = min(bx, dims.x - bx) + min(by, dims.y - by)
                plane_peers.append((-far, move(me, x=step("x", bx), y=step("y", by))))
    plane_peers = [p for _, p in sorted(plane_peers, key=lambda item: item[0])]
    corners = []
    for bx in range(1, dims.x):
        for by in range(1, dims.y):
            corners.append(move(me, x=step("x", bx), y=step("y", by)))
    pole_peers = []
    for bz in far_first(size["z"]) + [0]:
        for c in (core, 1 - core):
            if bz or c is not core:
                pole_peers.append(move(me, z=step("z", bz), c=c))
    peers = lines + corners + [other]

    barrier = pltpu.get_barrier_semaphore()
    for p in peers:
        pl.semaphore_signal(barrier, inc=1, device_id=mesh_id(dims, p), device_id_type=MESH)

    loads = []
    for i, (src, dst) in enumerate(
        ((pivots_in, pivots), (prior_in, prior), (finished_in, finished),
         (pairs_in, pairs), (occupied_in, occupied))
    ):
        copy = pltpu.make_async_copy(src, dst, load.at[i])
        copy.start()
        loads.append(copy)

    def remote(src, dst, send, recv, p):
        copy = pltpu.make_async_remote_copy(
            src_ref=src, dst_ref=dst, send_sem=send, recv_sem=recv,
            device_id=mesh_id(dims, p), device_id_type=MESH,
        )
        copy.start()

    def wait_bytes(ref, sem):
        pltpu.make_async_copy(ref, ref, sem).wait()

    loads[0].wait()
    piv_row = jnp.broadcast_to(pivots[...], (128, npiv))
    piv_col = piv_row.astype(F32).T.astype(I32)
    here = onehot(piv_col == own * plan.rows + iota((npiv, plan.rows), 1))
    has = nn(jnp.ones((32, npiv), BF), here)
    before = onehot(iota((plan.rows, plan.rows), 0) < iota((plan.rows, plan.rows), 1))
    rank = nn(has.astype(BF), before)
    q = iota((32, plan.rows), 0)
    wanted = (mod(q, 4) - core * 2).astype(F32)
    select = jnp.where((has > 0.5) & (rank == wanted), 1.0, 0.0).astype(BF)
    loads[1].wait()
    for h in range(2):
        for u, unit in enumerate(plan.units):
            k0 = (h * plan.kt_half + unit["first"]) * 128
            rows = nn(select, prior[:, k0 : k0 + unit["tiles"] * 128])
            r1 = unit["r1"]
            part = jnp.zeros((r1, 128), F32)
            which = div(iota((r1, 128), 0), 4)
            for kt in range(unit["tiles"]):
                part = jnp.where(which == kt, rows[:r1, kt * 128 : (kt + 1) * 128], part)
            first_out[u][h] = part.astype(BF)
    for u, unit in enumerate(plan.units):
        first_in[u][me[unit["order"][0]] * dims.c + core] = first_out[u][core]

    loads[2].wait()
    r = iota((n, n), 0)
    v = coordinates(dims, iota((n, n), 1))
    spot = ((v["x"] * dims.y + v["y"]) * size["z"] + v["z"]) * dims.c + v["c"]
    a_rows = nt(onehot(r == spot), finished[...]).astype(BF)
    for i in range(plan.plane):
        a_out[i] = a_rows[i * plan.pole : (i + 1) * plan.pole]
    my_plane = me["x"] * dims.y + me["y"]
    my_pole = me["z"] * dims.c + core
    a_in[my_plane] = a_out[my_plane]

    pl.semaphore_wait(barrier, len(peers))

    for u, unit in enumerate(plan.units):
        axis = unit["order"][0]
        for by in far_first(size[axis]) + [0]:
            for c in (core, 1 - core):
                if by or c is not core:
                    remote(
                        first_out[u].at[c], first_in[u].at[me[axis] * dims.c + core],
                        send1.at[u], recv1.at[u], move(me, **{axis: step(axis, by), "c": c}),
                    )
    for p in plane_peers:
        remote(a_out.at[p["x"] * dims.y + p["y"]], a_in.at[my_plane], send_a, recv_a, p)
    half = plan.kt_half * 128
    remote(
        prior.at[:, pl.ds(pl.multiple_of((1 - core) * half, half), half)],
        partner_prior, send_p, recv_p, other,
    )

    loads[3].wait()
    flat = pairs[...].astype(F32)
    first = jnp.floor((flat + 0.5) * (1.0 / NAO)).astype(I32)
    second = pairs[...] - first * NAO
    row_block = first >> 7
    lane[...] = second & 127
    line[...] = (
        row_block * (row_block + 1) * 64 + (first & 127) * (row_block + 1) + (second >> 7)
    )
    blocks = n // 2
    total = slots.shape[0]
    last = jnp.broadcast_to(line[:, 127:128], (n, 128)) >> log2(GROUP)
    done = (mod(iota((n, 128), 0), 2) == 1) & (last <= iota((n, 128), 1))
    count = jnp.sum(jnp.where(done, 1.0, 0.0), axis=0, keepdims=True)
    leave = jnp.minimum(count, blocks - 1.0) + iota((1, 128), 1).astype(F32)
    leave_col = jnp.broadcast_to(leave, (128, 128)).T
    real = iota((128, 128), 0) < GROUPS
    rows = [leave]
    for t0 in (0, 128):
        past = real & (leave_col < (iota((128, 128), 1) + t0).astype(F32))
        rows.append(jnp.sum(jnp.where(past, 1.0, 0.0), axis=0, keepdims=True))
    which = iota((8, 128), 0)
    packed = jnp.zeros((8, 128), F32)
    for i, row in enumerate(rows):
        packed = jnp.where(which == i, jnp.broadcast_to(row, (8, 128)), packed)
    table[...] = packed.astype(I32)
    copy = pltpu.make_async_copy(table, steps_at, table_sem)
    copy.start()

    lanes = iota((128, 128), 0)
    places = iota((GROUP, 128), 0)

    def make_masks(it, carry):
        for k in range(MASK_UNROLL):
            d = it * MASK_UNROLL + k
            masks[d] = onehot(lanes == lane[pl.ds(d, 1), :]).T
        return carry

    def at_step(t):
        g = steps_at[1 + div(t, 128), mod(t, 128)]
        return g, jnp.clip(t - g, 0, blocks - 1)

    def make_wheres(it, carry):
        for k in range(WHERE_UNROLL):
            t = it * WHERE_UNROLL + k
            g, b = at_step(t)
            where = [
                onehot(places == line[pl.ds(2 * b + j, 1), :] - g * GROUP) for j in range(2)
            ]
            wheres[t] = jnp.concatenate(where, axis=1)
        return carry

    mask_steps = max(1, n // MASK_UNROLL)
    lax.fori_loop(0, mask_steps // 2, make_masks, 0)

    def block_of(u, i2):
        n1, n2, n3 = plan.units[u]["n"]
        base = pl.multiple_of((me[plan.units[u]["order"][2]] * n2 + i2) * (n1 * 4), n1 * 4)
        return gathered[u].at[:, pl.ds(base, n1 * 4)]

    def pass_on(u, i2):
        unit = plan.units[u]
        a3 = unit["order"][2]
        block = block_of(u, i2)
        for by in far_first(unit["n"][2]):
            remote(block, block, send3.at[u], recv3.at[u], move(me, **{a3: step(a3, by)}))

    for u, unit in enumerate(plan.units):
        n1, n2, n3 = unit["n"]
        a1, a2, a3 = unit["order"]
        r1, tiles = unit["r1"], unit["tiles"]
        wait_bytes(first_in[u].at[pl.ds(0, n1 * dims.c - 1)], recv1.at[u])
        got = first_in[u][...].reshape(n1 * dims.c * r1, 128)
        shape = (tiles * n1 * 4, n1 * dims.c * r1)
        ro, ci = iota(shape, 0), iota(shape, 1)
        kt, slot = div(ro, n1 * 4), mod(ro, 4)
        target = (mod(div(ro, 4), n1) * dims.c + div(slot, 2)) * r1 + kt * 4 + slot
        rows = nn(onehot(ci == target), got).astype(BF)
        base = pl.multiple_of((me[a3] * n2 + me[a2]) * (n1 * 4), n1 * 4)
        for t in range(tiles):
            gathered[u][t, pl.ds(base, n1 * 4)] = rows[t * n1 * 4 : (t + 1) * n1 * 4]
        block = block_of(u, me[a2])
        for by in far_first(n2):
            remote(
                block, block, send2.at[u], recv2.at[u, me[a2]], move(me, **{a2: step(a2, by)})
            )
        pass_on(u, me[a2])

    wait_bytes(a_in.at[pl.ds(0, plan.plane - 1)], recv_a)
    mixed = a_in[...].reshape(n, plan.rows)
    source = mod(r, plan.plane) * plan.pole + div(r, plan.plane)
    b_rows = nn(onehot(iota((n, n), 1) == source), mixed).astype(BF)
    for i in range(plan.pole):
        b_out[i] = b_rows[i * plan.plane : (i + 1) * plan.plane]
    b_in[my_pole] = b_out[my_pole]
    for p in pole_peers:
        remote(b_out.at[p["z"] * dims.c + p["c"]], b_in.at[my_pole], send_b, recv_b, p)

    copy.wait()
    lax.fori_loop(0, total // WHERE_UNROLL, make_wheres, 0)

    def pass_on_arrivals(u):
        unit = plan.units[u]
        a2 = unit["order"][1]
        for by in reversed(far_first(unit["n"][1])):
            i2 = step(a2, by)
            wait_bytes(block_of(u, i2), recv2.at[u, i2])
            pass_on(u, i2)

    pass_on_arrivals(0)
    pass_on_arrivals(2)
    lax.fori_loop(mask_steps // 2, mask_steps, make_masks, 0)

    lower = []
    for j0 in range(0, npiv, 128):
        pr = piv_row[:1, j0 : j0 + 128] if npiv >= 128 else piv_row[:1]
        pc = piv_col[:, : pr.shape[1]]
        lower.append(onehot((div(pc, plan.rows) == div(pr, plan.rows)) & (pr < pc)))
    lower = jnp.concatenate(lower, axis=1)
    place = nn(lower, jnp.ones((npiv, 128), BF)).astype(I32)
    o = coordinates(dims, div(piv_col, plan.rows))
    for u, unit in enumerate(plan.units):
        n1, n2, n3 = unit["n"]
        a1, a2, a3 = unit["order"]
        at = ((o[a3] * n2 + o[a2]) * n1 + o[a1]) * 4 + o["c"] * 2 + place
        pick = jnp.concatenate(
            [onehot(iota((npiv, 128), 1) + s == at) for s in range(0, plan.slots, 128)], axis=1
        )
        picks[u] = pick[:, : plan.slots]
    pass_on_arrivals(1)

    wait_bytes(b_in.at[pl.ds(0, plan.pole - 1)], recv_b)
    mixed = b_in[...].reshape(n, plan.rows)
    w = coordinates(dims, r)
    source = (w["z"] * dims.c + w["c"]) * plan.plane + w["x"] * dims.y + w["y"]
    vector[...] = nn(onehot(iota((n, n), 1) == source), mixed)

    def scatter(it, carry):
        acc, before = carry
        for k in range(UNROLL):
            t = it * UNROLL + k
            g, b = at_step(t)
            scale = [
                jnp.broadcast_to(vector[pl.ds(2 * b + j, 1), :], (GROUP, 128)).astype(BF)
                for j in range(2)
            ]
            left = wheres[t] * jnp.concatenate(scale, axis=1)
            right = masks[pl.ds(2 * b, 2)].reshape(BLOCK, 128)
            acc = jnp.where(g == before, acc, 0.0) + nn(left, right)
            slots[t] = acc
            before = g
        return acc, before

    lax.fori_loop(
        0, total // UNROLL, scatter, (jnp.zeros((GROUP, 128), F32), jnp.int32(-1))
    )
    for g in range(GROUPS):
        dense[g * GROUP : (g + 1) * GROUP, :] = slots[jnp.clip(steps_at[0, g], 0, total - 1)]

    same = iota((128, 128), 0) == iota((128, 128), 1)
    for big in range(7):
        height = min(128, NAO - big * 128)
        base = 64 * big * (big + 1)
        for c in range(big + 1):
            tile = dense[pl.ds(base + c, height, stride=big + 1), :]
            if height < 128:
                tile = jnp.concatenate([tile, jnp.zeros((128 - height, 128), F32)], axis=0)
            flip = tile.T
            if c == big:
                tile = jnp.where(same, tile, tile + flip)
            else:
                full[c * 128 : (c + 1) * 128, big * 128 : (big + 1) * 128] = flip.astype(BF)
            full[big * 128 : (big + 1) * 128, c * 128 : (c + 1) * 128] = tile.astype(BF)
    loads[4].wait()
    for big in range(7):
        height = min(128, NAO - big * 128)
        rows = nn(full[big * 128 : (big + 1) * 128, :NAO], occupied[...])
        halves[big * 128 : big * 128 + height, :] = rows[:height]

    wait_bytes(partner_prior, recv_p)
    theirs = jnp.zeros((plan.rows, npiv), F32)
    chosen = []
    for u in (0, 2, 1):
        unit = plan.units[u]
        n1, n2, n3 = unit["n"]
        tiles = unit["tiles"]
        wait_bytes(gathered[u].at[:, pl.ds(0, n2 * n1 * 4 * (n3 - 1))], recv3.at[u])
        rows = jnp.concatenate(
            [nn(picks[u], gathered[u][t]).astype(BF) for t in range(tiles)], axis=1
        )
        chosen.append((unit, rows))
        k0 = unit["first"] * 128
        theirs += nt(partner_prior[:, k0 : k0 + tiles * 128], rows)
    part_out[...] = theirs
    remote(part_out, part_in, send_q, recv_q, other)
    mine = jnp.zeros((plan.rows, npiv), F32)
    for unit, rows in chosen:
        at_k = pl.multiple_of(core * half + unit["first"] * 128, 128)
        mine += nt(prior[:, pl.ds(at_k, unit["tiles"] * 128)], rows)

    for u, unit in enumerate(plan.units):
        n1, n2, n3 = unit["n"]
        wait_bytes(first_in[u].at[pl.ds(0, n1 * dims.c - 1)], send1.at[u])
        wait_bytes(gathered[u].at[:, pl.ds(0, n1 * 4 * (n2 - 1))], send2.at[u])
        wait_bytes(gathered[u].at[:, pl.ds(0, n2 * n1 * 4 * (n3 - 1))], send3.at[u])
    wait_bytes(a_in.at[pl.ds(0, plan.plane - 1)], send_a)
    wait_bytes(b_in.at[pl.ds(0, plan.pole - 1)], send_b)
    wait_bytes(partner_prior, send_p)
    wait_bytes(part_in, recv_q)
    wait_bytes(part_out, send_q)
    out[...] = mine + part_in[...]


def run_kernel(plan, pivots, prior, finished, pairs, occupied):
    npiv = pivots.shape[0]
    vmem = pl.BlockSpec(memory_space=pltpu.VMEM)
    anywhere = pl.BlockSpec(memory_space=pl.ANY)
    dma = pltpu.SemaphoreType.DMA
    nu = len(plan.units)
    n, rows = plan.n, plan.rows
    blocks = n // 2
    total = steps_of(blocks)
    scratch = [
        pltpu.VMEM((1, npiv), I32),
        pltpu.VMEM(prior.shape, BF),
        pltpu.VMEM(finished.shape, BF),
        pltpu.VMEM((n, rows), I32),
        pltpu.VMEM(occupied.shape, BF),
    ]
    scratch += [pltpu.VMEM((2, u["r1"], 128), BF) for u in plan.units]
    scratch += [pltpu.VMEM((u["n"][0] * plan.dims.c, u["r1"], 128), BF) for u in plan.units]
    scratch += [pltpu.VMEM((u["tiles"], plan.slots, 128), BF) for u in plan.units]
    scratch += [
        pltpu.VMEM((rows, plan.kt_half * 128), BF),
        pltpu.VMEM((rows, npiv), F32),
        pltpu.VMEM((rows, npiv), F32),
        pltpu.VMEM((plan.plane, plan.pole, rows), BF),
        pltpu.VMEM((plan.plane, plan.pole, rows), BF),
        pltpu.VMEM((plan.pole, plan.plane, rows), BF),
        pltpu.VMEM((plan.pole, plan.plane, rows), BF),
        pltpu.VMEM((n, 128), I32),
        pltpu.VMEM((n, 128), I32),
        pltpu.VMEM((n, 128), F32),
        pltpu.VMEM((8, 128), I32),
        pltpu.VMEM((n, 128, 128), BF),
        pltpu.VMEM((total, GROUP, BLOCK), BF),
        pltpu.VMEM((total, GROUP, 128), F32),
        pltpu.VMEM((GROUPS * GROUP, 128), F32),
        pltpu.VMEM((896, 896), BF),
        pltpu.VMEM((nu, npiv, plan.slots), BF),
        pltpu.SMEM((8, 128), I32),
    ]
    scratch += [dma((5,)), dma((nu,)), dma((nu,)), dma((nu,)), dma((nu, 8))]
    scratch += [dma((nu,)), dma((nu,))] + [dma] * 9
    return pl.pallas_call(
        functools.partial(fused_kernel, plan),
        out_shape=(
            pltpu.VMEM((rows, npiv), F32),
            pltpu.VMEM((NAO, occupied.shape[1]), F32),
        ),
        in_specs=[anywhere] * 5,
        out_specs=(vmem, vmem),
        scratch_shapes=scratch,
        compiler_params=pltpu.CompilerParams(
            collective_id=0, has_side_effects=True, vmem_limit_bytes=56 * 1024 * 1024
        ),
        name="fused",
    )(pivots.reshape(1, npiv), prior, finished, pairs.reshape(n, rows), occupied)


def finish_kernel(panel, product, flipped, updated, halves, result, sems):
    first = pltpu.make_async_copy(flipped, halves, sems.at[0])
    first.start()
    result[...] = panel[...] - product[...]
    second = pltpu.make_async_copy(result, updated, sems.at[1])
    second.start()
    first.wait()
    second.wait()


def finish(panel, product, flipped):
    vmem = pl.BlockSpec(memory_space=pltpu.VMEM)
    hbm = pl.BlockSpec(memory_space=pltpu.HBM)
    return pl.pallas_call(
        finish_kernel,
        out_shape=(pltpu.HBM(panel.shape, F32), pltpu.HBM(flipped.shape, F32)),
        in_specs=[vmem] * 3,
        out_specs=(hbm, hbm),
        scratch_shapes=[pltpu.VMEM(panel.shape, F32), pltpu.SemaphoreType.DMA((2,))],
        compiler_params=pltpu.CompilerParams(vmem_limit_bytes=4 * 1024 * 1024),
        name="finish",
    )(panel, product, flipped)


def per_device(dims, pivots, panel, prior, finished, pairs, occupied):
    plan = Plan(dims, prior.shape[1], prior.shape[0])
    product, flipped = run_kernel(plan, pivots, prior, finished, pairs, occupied)
    updated, flipped = finish(panel, product, flipped)
    return updated, flipped.T[None]


def build(mesh, dims):
    return jax.shard_map(
        functools.partial(per_device, dims),
        mesh=mesh,
        in_specs=(
            P(),
            P(("row", "col"), None),
            P(("row", "col"), None),
            P(("row", "col"), None),
            P(),
            P(),
        ),
        out_specs=(P(("row", "col"), None), P(("row", "col"), None, None)),
        check_vma=False,
    )


def solution(mesh):
    return build(mesh, FULL)
```

```python
import functools
import math
from collections import namedtuple

import jax
import jax.numpy as jnp
from jax import lax
from jax.experimental import pallas as pl
from jax.experimental.pallas import tpu as pltpu
from jax.sharding import PartitionSpec as P

MESH = pl.DeviceIdType.MESH
BF, F32, I32 = jnp.bfloat16, jnp.float32, jnp.int32
Dims = namedtuple("Dims", ("x", "y", "zh", "zl", "c"))
FULL = Dims(4, 4, 4, 2, 2)

NAO = 800
GROUP = 64
BLOCK = 256
GROUPS = 46
UNROLL = 22
WHERE_UNROLL = 8
MASK_UNROLL = 16

UNIT_TILES = (2, 5, 5)
UNIT_ORDERS = (("x", "y", "z"), ("y", "z", "x"), ("z", "x", "y"))


def nt(a, b):
    return lax.dot_general(a, b, (((1,), (1,)), ((), ())), preferred_element_type=F32)


def nn(a, b):
    return lax.dot_general(a, b, (((1,), (0,)), ((), ())), preferred_element_type=F32)


def iota(shape, dim):
    return lax.broadcasted_iota(I32, shape, dim)


def log2(n):
    assert n & (n - 1) == 0
    return n.bit_length() - 1


def mod(v, n):
    return v & (n - 1)


def div(v, n):
    return v >> log2(n)


def onehot(cond):
    return jnp.where(cond, 1.0, 0.0).astype(BF)


def coordinates(dims, device):
    col = mod(device, dims.y * dims.zl)
    row = div(device, dims.y * dims.zl)
    core = mod(row, dims.c)
    x = mod(div(row, dims.c), dims.x)
    zh = div(row, dims.c * dims.x)
    return dict(x=x, y=div(col, dims.zl), z=zh * dims.zl + mod(col, dims.zl), c=core)


def mesh_id(dims, p):
    row = (div(p["z"], dims.zl) * dims.x + p["x"]) * dims.c + p["c"]
    col = p["y"] * dims.zl + mod(p["z"], dims.zl)
    return (row, col)


class Plan:
    def __init__(self, dims, k, rows):
        self.dims = dims
        self.size = dict(x=dims.x, y=dims.y, z=dims.zh * dims.zl, c=dims.c)
        self.n = dims.x * dims.y * dims.zh * dims.zl * dims.c
        self.slots = 2 * self.n
        self.kt_half = k // 128 // 2
        self.rows = rows
        self.units = []
        first = 0
        for tiles, order in zip(UNIT_TILES, UNIT_ORDERS):
            self.units.append(
                dict(
                    tiles=tiles,
                    first=first,
                    order=order,
                    r1=-(-4 * tiles // 8) * 8,
                    n=[self.size[a] for a in order],
                )
            )
            first += tiles
        assert first == self.kt_half
        self.plane = dims.x * dims.y
        self.pole = self.size["z"] * dims.c


def move(me, **changes):
    return {**me, **changes}


def steps_of(blocks):
    both = UNROLL * WHERE_UNROLL // math.gcd(UNROLL, WHERE_UNROLL)
    return -(-(GROUPS + blocks - 1) // both) * both


def far_first(count):
    return sorted(range(1, count), key=lambda by: (-min(by, count - by), by))


def fused_kernel(plan, *refs):
    dims, size, n = plan.dims, plan.size, plan.n
    nu = len(plan.units)
    (pivots_in, prior_in, finished_in, pairs_in, occupied_in, out, halves) = refs[:7]
    scratch = list(refs[7:])
    take = lambda count: [scratch.pop(0) for _ in range(count)]
    (pivots, prior, finished, pairs, occupied) = take(5)
    first_out = take(nu)
    first_in = take(nu)
    gathered = take(nu)
    (partner_prior, part_out, part_in, a_out, a_in, b_out, b_in) = take(7)
    (lane, line, vector, table, masks, wheres, slots, dense, full, picks, steps_at) = take(11)
    (load, send1, recv1, send2, recv2, send3, recv3, send_a, recv_a, send_b, recv_b,
     send_p, recv_p, send_q, recv_q, table_sem) = take(16)

    own = lax.axis_index("row") * (dims.y * dims.zl) + lax.axis_index("col")
    me = coordinates(dims, own)
    core = me["c"]
    other = move(me, c=1 - core)
    npiv = pivots.shape[1]

    def step(axis, by):
        return mod(me[axis] + by, size[axis])

    lines = []
    for axis in ("x", "y", "z"):
        for by in range(1, size[axis]):
            for c in (core, 1 - core):
                lines.append(move(me, **{axis: step(axis, by), "c": c}))
    plane_peers = []
    for bx in range(dims.x):
        for by in range(dims.y):
            if bx or by:
                far = min(bx, dims.x - bx) + min(by, dims.y - by)
                plane_peers.append((-far, move(me, x=step("x", bx), y=step("y", by))))
    plane_peers = [p for _, p in sorted(plane_peers, key=lambda item: item[0])]
    corners = []
    for bx in range(1, dims.x):
        for by in range(1, dims.y):
            corners.append(move(me, x=step("x", bx), y=step("y", by)))
    pole_peers = []
    for bz in far_first(size["z"]) + [0]:
        for c in (core, 1 - core):
            if bz or c is not core:
                pole_peers.append(move(me, z=step("z", bz), c=c))
    peers = lines + corners + [other]

    barrier = pltpu.get_barrier_semaphore()
    for p in peers:
        pl.semaphore_signal(barrier, inc=1, device_id=mesh_id(dims, p), device_id_type=MESH)

    loads = []
    for i, (src, dst) in enumerate(
        ((pivots_in, pivots), (prior_in, prior), (finished_in, finished),
         (pairs_in, pairs), (occupied_in, occupied))
    ):
        copy = pltpu.make_async_copy(src, dst, load.at[i])
        copy.start()
        loads.append(copy)

    def remote(src, dst, send, recv, p):
        copy = pltpu.make_async_remote_copy(
            src_ref=src, dst_ref=dst, send_sem=send, recv_sem=recv,
            device_id=mesh_id(dims, p), device_id_type=MESH,
        )
        copy.start()

    def wait_bytes(ref, sem):
        pltpu.make_async_copy(ref, ref, sem).wait()

    loads[0].wait()
    piv_row = jnp.broadcast_to(pivots[...], (128, npiv))
    piv_col = piv_row.astype(F32).T.astype(I32)
    here = onehot(piv_col == own * plan.rows + iota((npiv, plan.rows), 1))
    has = nn(jnp.ones((32, npiv), BF), here)
    before = onehot(iota((plan.rows, plan.rows), 0) < iota((plan.rows, plan.rows), 1))
    rank = nn(has.astype(BF), before)
    q = iota((32, plan.rows), 0)
    wanted = (mod(q, 4) - core * 2).astype(F32)
    select = jnp.where((has > 0.5) & (rank == wanted), 1.0, 0.0).astype(BF)
    loads[1].wait()
    for h in range(2):
        for u, unit in enumerate(plan.units):
            k0 = (h * plan.kt_half + unit["first"]) * 128
            rows = nn(select, prior[:, k0 : k0 + unit["tiles"] * 128])
            r1 = unit["r1"]
            part = jnp.zeros((r1, 128), F32)
            which = div(iota((r1, 128), 0), 4)
            for kt in range(unit["tiles"]):
                part = jnp.where(which == kt, rows[:r1, kt * 128 : (kt + 1) * 128], part)
            first_out[u][h] = part.astype(BF)
    for u, unit in enumerate(plan.units):
        first_in[u][me[unit["order"][0]] * dims.c + core] = first_out[u][core]

    loads[2].wait()
    r = iota((n, n), 0)
    v = coordinates(dims, iota((n, n), 1))
    spot = ((v["x"] * dims.y + v["y"]) * size["z"] + v["z"]) * dims.c + v["c"]
    a_rows = nt(onehot(r == spot), finished[...]).astype(BF)
    for i in range(plan.plane):
        a_out[i] = a_rows[i * plan.pole : (i + 1) * plan.pole]
    my_plane = me["x"] * dims.y + me["y"]
    my_pole = me["z"] * dims.c + core
    a_in[my_plane] = a_out[my_plane]

    pl.semaphore_wait(barrier, len(peers))

    for u, unit in enumerate(plan.units):
        axis = unit["order"][0]
        for by in far_first(size[axis]) + [0]:
            for c in (core, 1 - core):
                if by or c is not core:
                    remote(
                        first_out[u].at[c], first_in[u].at[me[axis] * dims.c + core],
                        send1.at[u], recv1.at[u], move(me, **{axis: step(axis, by), "c": c}),
                    )
    for p in plane_peers:
        remote(a_out.at[p["x"] * dims.y + p["y"]], a_in.at[my_plane], send_a, recv_a, p)
    half = plan.kt_half * 128
    remote(
        prior.at[:, pl.ds(pl.multiple_of((1 - core) * half, half), half)],
        partner_prior, send_p, recv_p, other,
    )

    loads[3].wait()
    flat = pairs[...].astype(F32)
    first = jnp.floor((flat + 0.5) * (1.0 / NAO)).astype(I32)
    second = pairs[...] - first * NAO
    row_block = first >> 7
    lane[...] = second & 127
    line[...] = (
        row_block * (row_block + 1) * 64 + (first & 127) * (row_block + 1) + (second >> 7)
    )
    blocks = n // 2
    total = slots.shape[0]
    last = jnp.broadcast_to(line[:, 127:128], (n, 128)) >> log2(GROUP)
    done = (mod(iota((n, 128), 0), 2) == 1) & (last <= iota((n, 128), 1))
    count = jnp.sum(jnp.where(done, 1.0, 0.0), axis=0, keepdims=True)
    leave = jnp.minimum(count, blocks - 1.0) + iota((1, 128), 1).astype(F32)
    leave_col = jnp.broadcast_to(leave, (128, 128)).T
    real = iota((128, 128), 0) < GROUPS
    rows = [leave]
    for t0 in (0, 128):
        past = real & (leave_col < (iota((128, 128), 1) + t0).astype(F32))
        rows.append(jnp.sum(jnp.where(past, 1.0, 0.0), axis=0, keepdims=True))
    which = iota((8, 128), 0)
    packed = jnp.zeros((8, 128), F32)
    for i, row in enumerate(rows):
        packed = jnp.where(which == i, jnp.broadcast_to(row, (8, 128)), packed)
    table[...] = packed.astype(I32)
    copy = pltpu.make_async_copy(table, steps_at, table_sem)
    copy.start()

    lanes = iota((128, 128), 0)
    places = iota((GROUP, 128), 0)

    def make_masks(it, carry):
        for k in range(MASK_UNROLL):
            d = it * MASK_UNROLL + k
            masks[d] = onehot(lanes == lane[pl.ds(d, 1), :]).T
        return carry

    def at_step(t):
        g = steps_at[1 + div(t, 128), mod(t, 128)]
        return g, jnp.clip(t - g, 0, blocks - 1)

    def make_wheres(it, carry):
        for k in range(WHERE_UNROLL):
            t = it * WHERE_UNROLL + k
            g, b = at_step(t)
            where = [
                onehot(places == line[pl.ds(2 * b + j, 1), :] - g * GROUP) for j in range(2)
            ]
            wheres[t] = jnp.concatenate(where, axis=1)
        return carry

    mask_steps = max(1, n // MASK_UNROLL)
    lax.fori_loop(0, mask_steps // 2, make_masks, 0)

    def block_of(u, i2):
        n1, n2, n3 = plan.units[u]["n"]
        base = pl.multiple_of((me[plan.units[u]["order"][2]] * n2 + i2) * (n1 * 4), n1 * 4)
        return gathered[u].at[:, pl.ds(base, n1 * 4)]

    def pass_on(u, i2):
        unit = plan.units[u]
        a3 = unit["order"][2]
        block = block_of(u, i2)
        for by in far_first(unit["n"][2]):
            remote(block, block, send3.at[u], recv3.at[u], move(me, **{a3: step(a3, by)}))

    def begin_second(u):
        unit = plan.units[u]
        n1, n2, n3 = unit["n"]
        a1, a2, a3 = unit["order"]
        r1, tiles = unit["r1"], unit["tiles"]
        wait_bytes(first_in[u].at[pl.ds(0, n1 * dims.c - 1)], recv1.at[u])
        got = first_in[u][...].reshape(n1 * dims.c * r1, 128)
        shape = (tiles * n1 * 4, n1 * dims.c * r1)
        ro, ci = iota(shape, 0), iota(shape, 1)
        kt, slot = div(ro, n1 * 4), mod(ro, 4)
        target = (mod(div(ro, 4), n1) * dims.c + div(slot, 2)) * r1 + kt * 4 + slot
        rows = nn(onehot(ci == target), got).astype(BF)
        base = pl.multiple_of((me[a3] * n2 + me[a2]) * (n1 * 4), n1 * 4)
        for t in range(tiles):
            gathered[u][t, pl.ds(base, n1 * 4)] = rows[t * n1 * 4 : (t + 1) * n1 * 4]
        block = block_of(u, me[a2])
        for by in far_first(n2):
            remote(
                block, block, send2.at[u], recv2.at[u, me[a2]], move(me, **{a2: step(a2, by)})
            )
        pass_on(u, me[a2])

    begin_second(1)
    begin_second(0)
    copy.wait()
    lax.fori_loop(0, total // WHERE_UNROLL, make_wheres, 0)
    begin_second(2)

    wait_bytes(a_in.at[pl.ds(0, plan.plane - 1)], recv_a)
    mixed = a_in[...].reshape(n, plan.rows)
    source = mod(r, plan.plane) * plan.pole + div(r, plan.plane)
    b_rows = nn(onehot(iota((n, n), 1) == source), mixed).astype(BF)
    for i in range(plan.pole):
        b_out[i] = b_rows[i * plan.plane : (i + 1) * plan.plane]
    b_in[my_pole] = b_out[my_pole]
    for p in pole_peers:
        remote(b_out.at[p["z"] * dims.c + p["c"]], b_in.at[my_pole], send_b, recv_b, p)

    def pass_on_arrivals(u, first, last):
        unit = plan.units[u]
        a2 = unit["order"][1]
        for by in list(reversed(far_first(unit["n"][1])))[first:last]:
            i2 = step(a2, by)
            wait_bytes(block_of(u, i2), recv2.at[u, i2])
            pass_on(u, i2)

    pass_on_arrivals(0, 0, 8)
    pass_on_arrivals(1, 0, 4)
    lax.fori_loop(mask_steps // 2, mask_steps, make_masks, 0)
    pass_on_arrivals(2, 0, 8)
    pass_on_arrivals(1, 4, 8)

    lower = []
    for j0 in range(0, npiv, 128):
        pr = piv_row[:1, j0 : j0 + 128] if npiv >= 128 else piv_row[:1]
        pc = piv_col[:, : pr.shape[1]]
        lower.append(onehot((div(pc, plan.rows) == div(pr, plan.rows)) & (pr < pc)))
    lower = jnp.concatenate(lower, axis=1)
    place = nn(lower, jnp.ones((npiv, 128), BF)).astype(I32)
    o = coordinates(dims, div(piv_col, plan.rows))
    for u, unit in enumerate(plan.units):
        n1, n2, n3 = unit["n"]
        a1, a2, a3 = unit["order"]
        at = ((o[a3] * n2 + o[a2]) * n1 + o[a1]) * 4 + o["c"] * 2 + place
        pick = jnp.concatenate(
            [onehot(iota((npiv, 128), 1) + s == at) for s in range(0, plan.slots, 128)], axis=1
        )
        picks[u] = pick[:, : plan.slots]
    wait_bytes(b_in.at[pl.ds(0, plan.pole - 1)], recv_b)
    mixed = b_in[...].reshape(n, plan.rows)
    w = coordinates(dims, r)
    source = (w["z"] * dims.c + w["c"]) * plan.plane + w["x"] * dims.y + w["y"]
    vector[...] = nn(onehot(iota((n, n), 1) == source), mixed)

    def scatter(it, carry):
        acc, before = carry
        for k in range(UNROLL):
            t = it * UNROLL + k
            g, b = at_step(t)
            scale = [
                jnp.broadcast_to(vector[pl.ds(2 * b + j, 1), :], (GROUP, 128)).astype(BF)
                for j in range(2)
            ]
            left = wheres[t] * jnp.concatenate(scale, axis=1)
            right = masks[pl.ds(2 * b, 2)].reshape(BLOCK, 128)
            acc = jnp.where(g == before, acc, 0.0) + nn(left, right)
            slots[t] = acc
            before = g
        return acc, before

    lax.fori_loop(
        0, total // UNROLL, scatter, (jnp.zeros((GROUP, 128), F32), jnp.int32(-1))
    )
    for g in range(GROUPS):
        dense[g * GROUP : (g + 1) * GROUP, :] = slots[jnp.clip(steps_at[0, g], 0, total - 1)]

    same = iota((128, 128), 0) == iota((128, 128), 1)
    for big in range(7):
        height = min(128, NAO - big * 128)
        base = 64 * big * (big + 1)
        for c in range(big + 1):
            tile = dense[pl.ds(base + c, height, stride=big + 1), :]
            if height < 128:
                tile = jnp.concatenate([tile, jnp.zeros((128 - height, 128), F32)], axis=0)
            flip = tile.T
            if c == big:
                tile = jnp.where(same, tile, tile + flip)
            else:
                full[c * 128 : (c + 1) * 128, big * 128 : (big + 1) * 128] = flip.astype(BF)
            full[big * 128 : (big + 1) * 128, c * 128 : (c + 1) * 128] = tile.astype(BF)
    loads[4].wait()
    for big in range(7):
        height = min(128, NAO - big * 128)
        rows = nn(full[big * 128 : (big + 1) * 128, :NAO], occupied[...])
        halves[big * 128 : big * 128 + height, :] = rows[:height]

    wait_bytes(partner_prior, recv_p)
    theirs = jnp.zeros((plan.rows, npiv), F32)
    chosen = []
    for u in (0, 2, 1):
        unit = plan.units[u]
        n1, n2, n3 = unit["n"]
        tiles = unit["tiles"]
        wait_bytes(gathered[u].at[:, pl.ds(0, n2 * n1 * 4 * (n3 - 1))], recv3.at[u])
        rows = jnp.concatenate(
            [nn(picks[u], gathered[u][t]).astype(BF) for t in range(tiles)], axis=1
        )
        chosen.append((unit, rows))
        k0 = unit["first"] * 128
        theirs += nt(partner_prior[:, k0 : k0 + tiles * 128], rows)
    part_out[...] = theirs
    remote(part_out, part_in, send_q, recv_q, other)
    mine = jnp.zeros((plan.rows, npiv), F32)
    for unit, rows in chosen:
        at_k = pl.multiple_of(core * half + unit["first"] * 128, 128)
        mine += nt(prior[:, pl.ds(at_k, unit["tiles"] * 128)], rows)

    for u, unit in enumerate(plan.units):
        n1, n2, n3 = unit["n"]
        wait_bytes(first_in[u].at[pl.ds(0, n1 * dims.c - 1)], send1.at[u])
        wait_bytes(gathered[u].at[:, pl.ds(0, n1 * 4 * (n2 - 1))], send2.at[u])
        wait_bytes(gathered[u].at[:, pl.ds(0, n2 * n1 * 4 * (n3 - 1))], send3.at[u])
    wait_bytes(a_in.at[pl.ds(0, plan.plane - 1)], send_a)
    wait_bytes(b_in.at[pl.ds(0, plan.pole - 1)], send_b)
    wait_bytes(partner_prior, send_p)
    wait_bytes(part_in, recv_q)
    wait_bytes(part_out, send_q)
    out[...] = mine + part_in[...]


def run_kernel(plan, pivots, prior, finished, pairs, occupied):
    npiv = pivots.shape[0]
    vmem = pl.BlockSpec(memory_space=pltpu.VMEM)
    anywhere = pl.BlockSpec(memory_space=pl.ANY)
    dma = pltpu.SemaphoreType.DMA
    nu = len(plan.units)
    n, rows = plan.n, plan.rows
    blocks = n // 2
    total = steps_of(blocks)
    scratch = [
        pltpu.VMEM((1, npiv), I32),
        pltpu.VMEM(prior.shape, BF),
        pltpu.VMEM(finished.shape, BF),
        pltpu.VMEM((n, rows), I32),
        pltpu.VMEM(occupied.shape, BF),
    ]
    scratch += [pltpu.VMEM((2, u["r1"], 128), BF) for u in plan.units]
    scratch += [pltpu.VMEM((u["n"][0] * plan.dims.c, u["r1"], 128), BF) for u in plan.units]
    scratch += [pltpu.VMEM((u["tiles"], plan.slots, 128), BF) for u in plan.units]
    scratch += [
        pltpu.VMEM((rows, plan.kt_half * 128), BF),
        pltpu.VMEM((rows, npiv), F32),
        pltpu.VMEM((rows, npiv), F32),
        pltpu.VMEM((plan.plane, plan.pole, rows), BF),
        pltpu.VMEM((plan.plane, plan.pole, rows), BF),
        pltpu.VMEM((plan.pole, plan.plane, rows), BF),
        pltpu.VMEM((plan.pole, plan.plane, rows), BF),
        pltpu.VMEM((n, 128), I32),
        pltpu.VMEM((n, 128), I32),
        pltpu.VMEM((n, 128), F32),
        pltpu.VMEM((8, 128), I32),
        pltpu.VMEM((n, 128, 128), BF),
        pltpu.VMEM((total, GROUP, BLOCK), BF),
        pltpu.VMEM((total, GROUP, 128), F32),
        pltpu.VMEM((GROUPS * GROUP, 128), F32),
        pltpu.VMEM((896, 896), BF),
        pltpu.VMEM((nu, npiv, plan.slots), BF),
        pltpu.SMEM((8, 128), I32),
    ]
    scratch += [dma((5,)), dma((nu,)), dma((nu,)), dma((nu,)), dma((nu, 8))]
    scratch += [dma((nu,)), dma((nu,))] + [dma] * 9
    return pl.pallas_call(
        functools.partial(fused_kernel, plan),
        out_shape=(
            pltpu.VMEM((rows, npiv), F32),
            pltpu.VMEM((NAO, occupied.shape[1]), F32),
        ),
        in_specs=[anywhere] * 5,
        out_specs=(vmem, vmem),
        scratch_shapes=scratch,
        compiler_params=pltpu.CompilerParams(
            collective_id=0, has_side_effects=True, vmem_limit_bytes=56 * 1024 * 1024
        ),
        name="fused",
    )(pivots.reshape(1, npiv), prior, finished, pairs.reshape(n, rows), occupied)


def finish_kernel(panel, product, flipped, updated, halves, result, sems):
    first = pltpu.make_async_copy(flipped, halves, sems.at[0])
    first.start()
    result[...] = panel[...] - product[...]
    second = pltpu.make_async_copy(result, updated, sems.at[1])
    second.start()
    first.wait()
    second.wait()


def finish(panel, product, flipped):
    vmem = pl.BlockSpec(memory_space=pltpu.VMEM)
    hbm = pl.BlockSpec(memory_space=pltpu.HBM)
    return pl.pallas_call(
        finish_kernel,
        out_shape=(pltpu.HBM(panel.shape, F32), pltpu.HBM(flipped.shape, F32)),
        in_specs=[vmem] * 3,
        out_specs=(hbm, hbm),
        scratch_shapes=[pltpu.VMEM(panel.shape, F32), pltpu.SemaphoreType.DMA((2,))],
        compiler_params=pltpu.CompilerParams(vmem_limit_bytes=4 * 1024 * 1024),
        name="finish",
    )(panel, product, flipped)


def per_device(dims, pivots, panel, prior, finished, pairs, occupied):
    plan = Plan(dims, prior.shape[1], prior.shape[0])
    product, flipped = run_kernel(plan, pivots, prior, finished, pairs, occupied)
    updated, flipped = finish(panel, product, flipped)
    return updated, flipped.T[None]


def build(mesh, dims):
    return jax.shard_map(
        functools.partial(per_device, dims),
        mesh=mesh,
        in_specs=(
            P(),
            P(("row", "col"), None),
            P(("row", "col"), None),
            P(("row", "col"), None),
            P(),
            P(),
        ),
        out_specs=(P(("row", "col"), None), P(("row", "col"), None, None)),
        check_vma=False,
    )


def solution(mesh):
    return build(mesh, FULL)
```
